32 devices in a mesh: dp: 8 (over y, x, core), rep: 4 (over z).
Axes of the slice: x: 2, y: 2, z: 4, core: 2. Of those that a mesh axis runs over, the one named last changes fastest.
Arguments:
- tokens: bfloat16 [4096, 2048], P(('dp', 'rep')), may hold values from -6 to 6
- cotangent: bfloat16 [4096, 2048], P(('dp', 'rep')), may hold values from -0.125 to 0.125
- doc_ids: int32 [64, 64], P(('dp', 'rep')), may hold values from 0 to 3, never falling along the last dimension, each value on 1 to 32 neighbouring positions
- valid_len: int32 [64], P(('dp', 'rep')), may hold values from 16 to 64
- w_qkv: bfloat16 [2048, 384], P('dp'), may hold values from -0.125 to 0.125
- w_out: bfloat16 [2048, 128], P('dp'), may hold values from -0.5 to 0.5
- norm_gain: bfloat16 [2048], P('dp'), may hold values from 0.5 to 1.5
Outputs:
- grad_qkv: float32 [2048, 384], P('dp')
- grad_out: float32 [2048, 128], P('dp')
- grad_gain: float32 [2048], P('dp')
The draws below stay inside these ranges and needn't reach their ends.
Inputs may be any that keep to these rules, and one draw needn't show every extreme that they name: `doc_ids`: within each row of 64 positions the ids never fall, and a document has 1 to 32 positions.
All inputs are finite; a program needn't handle non-finite values.
Results may differ from the reference program's by a relative error of at most 0.0079.
Values may be sent and summed in bfloat16 or wider, within the bound.
A program may use at most 64 MiB of HBM per device.

```python
import math
import jax
import jax.numpy as jnp
import numpy as np
from jax import lax

D = 2048
HD = 128
SEQ = 64
DOCS = 4
SAMPLES = 64
TOKENS = 4096
N_REP = 4


def touch_ends(entries, rng, least, largest):
    shape = entries.shape
    place = [jax.random.randint(jax.random.fold_in(rng, axis), (), 0, shape[axis]) for axis in range(len(shape))]
    entries = entries.at[tuple(place)].set(least)
    longest = shape.index(max(shape))
    place[longest] = (place[longest] + 1) % shape[longest]
    return entries.at[tuple(place)].set(largest)


def with_spikes(values, rng, source, target, blocks, factor):
    def block_of(dim):
        return (jnp.arange(values.shape[dim]) // (values.shape[dim] // blocks)).reshape((-1,) + (1,) * (values.ndim - 1 - dim))

    first = jax.random.permutation(rng, blocks)[block_of(target)]
    far = (block_of(target) + blocks // 2) % blocks
    return jnp.where((block_of(source) == first) | (block_of(source) == far), factor * values, values)


def shard_levels(stream_key, extent, split, low, top_value):
    def one(position, parts):
        heights = jax.random.uniform(jax.random.fold_in(jax.random.fold_in(stream_key, 6), position), (parts,), jnp.float32, low / len(split), top_value / len(split))
        return jnp.repeat(jnp.exp(heights), extent[position] // parts).reshape((-1,) + (1,) * (len(extent) - position - 1))

    factor_of = one(*split[0])
    for cut in split[1:]:
        factor_of = factor_of * one(*cut)
    return factor_of


def split_up(count, total, reach, skew):
    loads = [(1 << 20) // math.isqrt(standing ** skew) + 1 for standing in range(2, count + 1)]
    surplus, counts = total - reach - (count - 1), [1] * (count - 1)
    while surplus > 0:
        free = [i for i in range(count - 1) if counts[i] < reach]
        pool, remaining = sum([loads[i] for i in free]), surplus
        for i in free:
            addition = min(reach - counts[i], max(1, remaining * loads[i] // pool), surplus)
            counts[i] = counts[i] + addition
            surplus = surplus - addition
    return np.array([reach] + counts)


def ragged_sizes(key, count, total, reach, skew):
    if count == 2:
        one = jax.random.randint(key, (), max(1, total - reach), min(reach, total - 1) + 1)
        return jnp.stack([one, total - one])
    lengths = jnp.asarray(split_up(count, total, reach, skew), jnp.int32)
    twos = (count - 1) // 2
    donor, taker = lengths[1:1 + 2 * twos:2], lengths[2:2 + 2 * twos:2]
    room = jnp.minimum(donor - 1, reach - taker)
    moved = jax.random.randint(jax.random.fold_in(key, 1), (twos,), 0, 1 << 20) % (room + 1)
    lengths = lengths.at[1:1 + 2 * twos:2].set(donor - moved).at[2:2 + 2 * twos:2].set(taker + moved)
    return lengths[jax.random.permutation(jax.random.fold_in(key, 2), count)]


def centred(rng, dims, deviation, most, split=(), kind=jnp.bfloat16):
    level = shard_levels(rng, dims, split, -0.22, 0.18) if split else 1.0
    array = jax.random.normal(rng, dims, jnp.float32) * deviation * level
    return jnp.minimum(jnp.maximum(array, -most), most).astype(kind)


def gaussian_with(own_key, shape, width, most, pieces, heavy, kind=jnp.bfloat16):
    values = width * jax.random.normal(own_key, shape, jnp.float32)
    if pieces:
        values = values * shard_levels(own_key, shape, pieces, -0.22, 0.18)
    return jnp.clip(with_spikes(values, jax.random.fold_in(own_key, 3), *heavy), -most, most).astype(kind)


def setup_inputs(seed: int = 0) -> dict:
    arg_keys = jax.random.split(jax.random.key(seed), 8)
    return {
        "tokens": gaussian_with(arg_keys[0], (TOKENS, D), 1.0, 6.0, ((0, 32),), (0, 1, 32, 2.75)),
        "cotangent": gaussian_with(arg_keys[1], (TOKENS, D), 0.01, 0.125, ((0, 32),), (0, 1, 32, 2.75)),
        "doc_ids": jax.vmap(lambda own: jnp.searchsorted(jnp.cumsum(ragged_sizes(own, DOCS, SEQ, SEQ // 2, 0)), jnp.arange(SEQ), side="right"))(jax.random.split(arg_keys[2], SAMPLES)).reshape((SAMPLES, SEQ)).astype(jnp.int32),
        "valid_len": touch_ends(jax.random.randint(arg_keys[3], (SAMPLES,), SEQ // 4, SEQ + 1), jax.random.fold_in(arg_keys[3], 1), SEQ // 4, SEQ).astype(jnp.int32),
        "w_qkv": centred(arg_keys[4], (D, 3 * HD), D ** -0.5, 0.125, ((0, 8),)),
        "w_out": centred(arg_keys[5], (D, HD), HD ** -0.5, 0.5, ((0, 8),)),
        "norm_gain": jnp.clip(1.0 + 0.1 * jax.random.normal(arg_keys[6], (D,), jnp.float32), 0.5, 1.5).astype(jnp.bfloat16),
    }


NORM_EPS = 1e-06
ROPE_BASE = 1000000.0

def rotate(vector):
    half_size = vector.shape[-1] // 2
    return jnp.concatenate([-vector[..., half_size:], vector[..., :half_size]], axis=-1)

def unrotate(vector):
    half_size = vector.shape[-1] // 2
    return jnp.concatenate([vector[..., half_size:], -vector[..., :half_size]], axis=-1)

def tables(doc_rows, head_size):
    seq_length = doc_rows.shape[1]
    earlier = lax.optimization_barrier(jnp.sum((doc_rows[:, None, :] < doc_rows[:, :, None]).astype(jnp.int32), axis=2))
    offsets = (jnp.arange(seq_length, dtype=jnp.int32)[None, :] - earlier).astype(jnp.float32)
    frequency = ROPE_BASE ** (-2.0 * jnp.arange(head_size // 2, dtype=jnp.float32) / head_size)
    angles = offsets[:, :, None] * frequency
    angles = jnp.concatenate([angles, angles], axis=2)
    return (jnp.cos(angles), jnp.sin(angles))

def reference(tokens, cotangent, doc_ids, valid_len, w_qkv, w_out, norm_gain):
    samples, seq_length = doc_ids.shape
    model_width = tokens.shape[1]
    inputs = tokens.reshape(samples, seq_length, model_width)
    grads_in = cotangent.reshape(samples, seq_length, model_width)
    scale = 1.0 / math.sqrt(HD)
    order_row = jnp.arange(seq_length, dtype=jnp.int32)[:, None]
    order_col = jnp.arange(seq_length, dtype=jnp.int32)[None, :]

    def step(totals, item):
        x_rows, dy_rows, doc_row, valid = item
        wide_in = x_rows.astype(jnp.float32)
        inverse_rms = lax.rsqrt(lax.optimization_barrier(jnp.mean(wide_in * wide_in, axis=1, keepdims=True)) + NORM_EPS)
        scaled_in = wide_in * inverse_rms
        normed = (scaled_in * norm_gain.astype(jnp.float32)).astype(jnp.bfloat16)
        projected = jnp.dot(normed, w_qkv, preferred_element_type=jnp.float32)
        cosine, sine_part = tables(doc_row[None, :], HD)
        cosine = cosine[0]
        sine_part = sine_part[0]
        queries = projected[:, :HD]
        keys_raw = projected[:, HD:2 * HD]
        values_raw = projected[:, 2 * HD:]
        query_rot = ((queries * cosine + rotate(queries) * sine_part) * scale).astype(jnp.bfloat16)
        key_rot = (keys_raw * cosine + rotate(keys_raw) * sine_part).astype(jnp.bfloat16)
        values = values_raw.astype(jnp.bfloat16)
        scores = jnp.dot(query_rot, key_rot.T, preferred_element_type=jnp.float32)
        allowed = (doc_row[:, None] == doc_row[None, :]) & (order_col <= order_row)
        raised = jnp.where(allowed, jnp.exp(scores), 0.0)
        probabilities = raised / lax.optimization_barrier(jnp.sum(raised, axis=1, keepdims=True))
        probs_low = probabilities.astype(jnp.bfloat16)
        attended = jnp.dot(probs_low, values, preferred_element_type=jnp.float32).astype(jnp.bfloat16)
        live_rows = jnp.arange(seq_length, dtype=jnp.int32) < valid
        live_dy = jnp.where(live_rows[:, None], dy_rows, jnp.zeros((), jnp.bfloat16))
        d_attended = jnp.dot(live_dy, w_out, preferred_element_type=jnp.float32).astype(jnp.bfloat16)
        d_probs = jnp.dot(d_attended, values.T, preferred_element_type=jnp.float32)
        d_values = jnp.dot(probs_low.T, d_attended, preferred_element_type=jnp.float32)
        d_scores = (probabilities * (d_probs - lax.optimization_barrier(jnp.sum(probabilities * d_probs, axis=1, keepdims=True)))).astype(jnp.bfloat16)
        d_query = jnp.dot(d_scores, key_rot, preferred_element_type=jnp.float32) * scale
        d_key = jnp.dot(d_scores.T, query_rot, preferred_element_type=jnp.float32)
        d_query = d_query * cosine + unrotate(d_query * sine_part)
        d_key = d_key * cosine + unrotate(d_key * sine_part)
        d_qkv = jnp.concatenate([d_query, d_key, d_values], axis=1).astype(jnp.bfloat16)
        d_normed = jnp.dot(d_qkv, w_qkv.T, preferred_element_type=jnp.float32)
        gain_term = lax.optimization_barrier(jnp.sum(d_normed * scaled_in, axis=0))
        new_totals = (totals[0] + jnp.dot(normed.T, d_qkv, preferred_element_type=jnp.float32), totals[1] + jnp.dot(live_dy.T, attended, preferred_element_type=jnp.float32), totals[2] + gain_term)
        return (new_totals, None)
    initial = (jnp.zeros((model_width, 3 * HD), jnp.float32), jnp.zeros((model_width, HD), jnp.float32), jnp.zeros((model_width,), jnp.float32))
    totals, _ = lax.scan(step, initial, (inputs, grads_in, doc_ids, valid_len))
    return (totals[0] / N_REP, totals[1] / N_REP, totals[2] / N_REP)
```

```python
import functools
import math

import jax
import jax.numpy as jnp
from jax import lax
from jax.experimental import pallas as pl
from jax.experimental.pallas import tpu as pltpu
from jax.sharding import PartitionSpec as P

NORM_EPS = 1e-06
ROPE_BASE = 1000000.0


def rotate(vector):
    half_size = vector.shape[-1] // 2
    return jnp.concatenate([-vector[..., half_size:], vector[..., :half_size]], axis=-1)


def unrotate(vector):
    half_size = vector.shape[-1] // 2
    return jnp.concatenate([vector[..., half_size:], -vector[..., :half_size]], axis=-1)


def tables(doc_rows, head_size):
    seq_length = doc_rows.shape[1]
    earlier = jnp.sum((doc_rows[:, None, :] < doc_rows[:, :, None]).astype(jnp.int32), axis=2)
    offsets = (jnp.arange(seq_length, dtype=jnp.int32)[None, :] - earlier).astype(jnp.float32)
    frequency = ROPE_BASE ** (-2.0 * jnp.arange(head_size // 2, dtype=jnp.float32) / head_size)
    angles = offsets[:, :, None] * frequency
    angles = jnp.concatenate([angles, angles], axis=2)
    return (jnp.cos(angles), jnp.sin(angles))


def forward_pass(inputs, doc_rows, w_qkv_full, gain_full):
    batches, seq_length, model_width = inputs.shape
    head_size = w_qkv_full.shape[1] // 3
    scale = 1.0 / math.sqrt(head_size)
    wide_in = inputs.astype(jnp.float32)
    inverse_rms = lax.rsqrt(jnp.mean(wide_in * wide_in, axis=2, keepdims=True) + NORM_EPS)
    scaled_in = wide_in * inverse_rms
    normed = (scaled_in * gain_full.astype(jnp.float32)).astype(jnp.bfloat16)
    projected = jnp.dot(
        normed.reshape(-1, model_width), w_qkv_full, preferred_element_type=jnp.float32
    )
    projected = projected.reshape(batches, seq_length, 3 * head_size)
    cosine, sine_part = tables(doc_rows, head_size)
    queries = projected[:, :, :head_size]
    keys_raw = projected[:, :, head_size : 2 * head_size]
    values_raw = projected[:, :, 2 * head_size :]
    query_rot = ((queries * cosine + rotate(queries) * sine_part) * scale).astype(jnp.bfloat16)
    key_rot = (keys_raw * cosine + rotate(keys_raw) * sine_part).astype(jnp.bfloat16)
    values = values_raw.astype(jnp.bfloat16)
    scores = jnp.einsum("msh,mth->mst", query_rot, key_rot, preferred_element_type=jnp.float32)
    order_row = jnp.arange(seq_length, dtype=jnp.int32)[:, None]
    order_col = jnp.arange(seq_length, dtype=jnp.int32)[None, :]
    allowed = (doc_rows[:, :, None] == doc_rows[:, None, :]) & (order_col <= order_row)[None]
    raised = jnp.where(allowed, jnp.exp(scores), 0.0)
    probabilities = raised / jnp.sum(raised, axis=2, keepdims=True)
    probs_low = probabilities.astype(jnp.bfloat16)
    attended = jnp.einsum(
        "mst,mth->msh", probs_low, values, preferred_element_type=jnp.float32
    ).astype(jnp.bfloat16)
    return (
        scaled_in,
        normed,
        query_rot,
        key_rot,
        values,
        probabilities,
        probs_low,
        attended,
        cosine,
        sine_part,
    )


def backward_pass(saved, live_dy, w_qkv_full, w_out_full):
    (
        scaled_in,
        normed,
        query_rot,
        key_rot,
        values,
        probabilities,
        probs_low,
        attended,
        cosine,
        sine_part,
    ) = saved
    batches, seq_length, model_width = live_dy.shape
    head_size = w_out_full.shape[1]
    scale = 1.0 / math.sqrt(head_size)
    d_attended = jnp.dot(
        live_dy.reshape(-1, model_width), w_out_full, preferred_element_type=jnp.float32
    )
    d_attended = d_attended.reshape(batches, seq_length, head_size).astype(jnp.bfloat16)
    d_probs = jnp.einsum("msh,mth->mst", d_attended, values, preferred_element_type=jnp.float32)
    d_values = jnp.einsum("mst,msh->mth", probs_low, d_attended, preferred_element_type=jnp.float32)
    d_scores = (
        probabilities * (d_probs - jnp.sum(probabilities * d_probs, axis=2, keepdims=True))
    ).astype(jnp.bfloat16)
    d_query = (
        jnp.einsum("mst,mth->msh", d_scores, key_rot, preferred_element_type=jnp.float32) * scale
    )
    d_key = jnp.einsum("mst,msh->mth", d_scores, query_rot, preferred_element_type=jnp.float32)
    d_query = d_query * cosine + unrotate(d_query * sine_part)
    d_key = d_key * cosine + unrotate(d_key * sine_part)
    d_qkv = jnp.concatenate([d_query, d_key, d_values], axis=2).astype(jnp.bfloat16)
    d_normed = lax.dot_general(
        d_qkv.reshape(-1, 3 * head_size),
        w_qkv_full,
        (((1,), (1,)), ((), ())),
        preferred_element_type=jnp.float32,
    )
    gain_term = jnp.sum(d_normed * scaled_in.reshape(-1, model_width), axis=0)
    return (d_qkv, gain_term)


def shards(tokens, cotangent, doc_ids, valid_len, w_qkv, w_out, norm_gain):
    batches, seq_length = doc_ids.shape
    model_width = tokens.shape[1]
    inputs = tokens.reshape(batches, seq_length, model_width)
    live_rows = jnp.arange(seq_length, dtype=jnp.int32)[None, :] < valid_len[:, None]
    live_dy = jnp.where(
        live_rows[:, :, None],
        cotangent.reshape(batches, seq_length, model_width),
        jnp.zeros((), jnp.bfloat16),
    )
    full_set = (
        lax.all_gather(w_qkv, "dp", axis=0, tiled=True),
        lax.all_gather(w_out, "dp", axis=0, tiled=True),
        lax.all_gather(norm_gain, "dp", axis=0, tiled=True),
    )
    saved = forward_pass(inputs, doc_ids, full_set[0], full_set[2])
    qkv_all, gain_total = backward_pass(saved, live_dy, full_set[0], full_set[1])
    normed_all = saved[1]
    attended_all = saved[7]
    head_size = w_out.shape[1]
    normed_flat = normed_all.reshape(-1, model_width)
    qkv_flat = qkv_all.reshape(-1, 3 * head_size)
    attended_flat = attended_all.reshape(-1, head_size)
    grad_qkv = lax.dot_general(
        normed_flat, qkv_flat, (((0,), (0,)), ((), ())), preferred_element_type=jnp.float32
    )
    grad_out = lax.dot_general(
        live_dy.reshape(-1, model_width),
        attended_flat,
        (((0,), (0,)), ((), ())),
        preferred_element_type=jnp.float32,
    )
    shares = (
        lax.psum_scatter(grad_qkv, "dp", scatter_dimension=0, tiled=True),
        lax.psum_scatter(grad_out, "dp", scatter_dimension=0, tiled=True),
    )
    shares = lax.psum((shares[0], shares[1]), "rep")
    gain_whole = lax.psum(gain_total, ("dp", "rep"))
    owned_rows = w_qkv.shape[0]
    gain_start = lax.axis_index("dp") * owned_rows
    gain_owned = lax.dynamic_slice_in_dim(gain_whole, gain_start, owned_rows, 0)
    replicas = lax.axis_size("rep")
    return (shares[0] / replicas, shares[1] / replicas, gain_owned / replicas)


MESH = pl.DeviceIdType.MESH
LANES = 128
CORES = 2


def mm(left, right, dims):
    return lax.dot_general(left, right, (dims, ((), ())), preferred_element_type=jnp.float32)


def eye(size):
    return lax.broadcasted_iota(jnp.int32, (size, size), 0) == lax.broadcasted_iota(
        jnp.int32, (size, size), 1
    )


def to_column(row):
    return jnp.sum(jnp.where(eye(row.shape[1]), row, 0.0), axis=1, keepdims=True)


def to_row(column):
    return jnp.sum(jnp.where(eye(column.shape[0]), column, 0.0), axis=0, keepdims=True)


def fused(
    n,
    replicas,
    x_hbm,
    dy_hbm,
    doc_hbm,
    valid_hbm,
    wq_hbm,
    wo_hbm,
    gain_hbm,
    gq_ref,
    go_ref,
    gg_ref,
    x_v,
    dy_v,
    doc_v,
    valid_s,
    gain_v,
    wq_all,
    wo_all,
    gain_all,
    normed,
    dy_sib,
    dy_turned,
    att,
    x_all,
    x_turned,
    yv_all,
    yqk_all,
    p_send,
    p_recv,
    zg_send,
    zg_recv,
    zg_all,
    zv_send,
    zv_recv,
    zv_all,
    zqk_send,
    zqk_recv,
    zqk_all,
    in_sem,
    w_send_sem,
    w_recv_sem,
    s_send_sem,
    s_recv_sem,
    a_send_sem,
    a_recv_sem,
    d_send_sem,
    d_recv_sem,
    p_send_sem,
    p_recv_sem,
    y_send_sem,
    y_recv_sem,
    r_send_sem,
    r_recv_sem,
    g_send_sem,
    g_recv_sem,
):
    me = lax.axis_index("dp")
    rep = lax.axis_index("rep")
    chip, core = me // CORES, lax.rem(me, CORES)
    sibling = chip * CORES + (1 - core)
    rows, width = x_v.shape
    owned = wq_hbm.shape[0]
    head = wo_hbm.shape[1]
    chips = n // CORES
    samples, seq = doc_v.shape
    piece = owned // replicas
    half_owned = owned // 2
    scale = 1.0 / math.sqrt(head)

    def block(index, size):
        return pl.ds(pl.multiple_of(index * size, LANES), size)

    loads = []
    for slot, (source, target) in enumerate(
        (
            (wq_hbm, wq_all.at[block(me, owned)]),
            (wo_hbm, wo_all.at[block(me, owned)]),
            (gain_hbm, gain_v),
            (x_hbm, x_v),
            (dy_hbm, dy_v),
            (doc_hbm, doc_v),
            (valid_hbm, valid_s),
        )
    ):
        load = pltpu.make_async_copy(source, target, in_sem.at[slot])
        load.start()
        loads.append(load)

    barrier = pltpu.get_barrier_semaphore()
    for off in range(1, n):
        pl.semaphore_signal(
            barrier, inc=1, device_id={"dp": lax.rem(me + off, n)}, device_id_type=MESH
        )
    for off in range(1, replicas):
        pl.semaphore_signal(
            barrier,
            inc=1,
            device_id={"rep": lax.rem(rep + off, replicas)},
            device_id_type=MESH,
        )

    pending = []

    def send(src, dst, send_sem, recv_sem, where):
        copy = pltpu.make_async_remote_copy(
            src_ref=src,
            dst_ref=dst,
            send_sem=send_sem,
            recv_sem=recv_sem,
            device_id=where,
            device_id_type=MESH,
        )
        copy.start()
        pending.append(copy)
        return copy

    along, across = lax.rem(chip, 2), chip // 2
    by_x = across * 2 + 1 - along
    by_y = (1 - across) * 2 + along
    first = by_x + core * (by_y - by_x)
    second = by_y + core * (by_x - by_y)
    far = 3 - chip
    owners = (
        first * CORES + core,
        second * CORES + core,
        far * CORES + core,
        sibling,
        second * CORES + 1 - core,
        first * CORES + 1 - core,
        far * CORES + 1 - core,
    )

    def w_part(owner, part):
        if part == 2:
            return wo_all.at[block(owner, owned)]
        start = pl.multiple_of(owner * owned + part * half_owned, LANES)
        return wq_all.at[pl.ds(start, half_owned)]

    def w_copy(owner, part, slot, device):
        source = w_part(owner, part)
        return send(
            source,
            source,
            w_send_sem.at[slot, part],
            w_recv_sem.at[slot, part],
            {"dp": device},
        )

    loads[2].wait()
    gain_row = gain_v[...].reshape(1, owned).astype(jnp.float32)
    gain_all[me] = jnp.broadcast_to(gain_row, gain_all.shape[1:])
    loads[0].wait()
    loads[1].wait()
    pl.semaphore_wait(barrier, n - 1 + replicas - 1)

    w = {}
    for part in range(2):
        w[0, part] = w_copy(me, part, 0, owners[0])
        w[1, part] = w_copy(me, part, 1, owners[1])
        w[3, part] = w_copy(me, part, 3, sibling)
    gains = {}
    for off in range(1, n):
        gains[off] = send(
            gain_all.at[me],
            gain_all.at[me],
            s_send_sem.at[off],
            s_recv_sem.at[off],
            {"dp": lax.rem(me + off, n)},
        )
    w[0, 2] = w_copy(me, 2, 0, owners[0])
    w[3, 2] = w_copy(me, 2, 3, sibling)

    loads[4].wait()
    crossed = []
    for place in range(chips):
        crossed.append(
            send(
                dy_v.at[:, block(place * CORES + 1 - core, owned)],
                dy_sib.at[place],
                d_send_sem.at[place],
                d_recv_sem.at[place],
                {"dp": sibling},
            )
        )

    loads[3].wait()
    loads[5].wait()
    loads[6].wait()
    gain_col = to_column(gain_row)
    wide_in = x_v[...].astype(jnp.float32)
    inverse = lax.rsqrt(
        jnp.sum(wide_in * wide_in, axis=1, keepdims=True) * (1.0 / width) + NORM_EPS
    )
    for off in range(1, n):
        gains[off].wait_recv()
    for place in range(n):
        cols = pl.ds(place * owned, owned)
        scaled = x_v[:, cols].astype(jnp.float32) * inverse
        normed[:, cols] = (scaled * gain_all[place][0:1]).astype(jnp.bfloat16)

    def times(source, total):
        product = mm(normed[:, block(source, owned)], wq_all[block(source, owned), :], ((1,), (0,)))
        return product if total is None else total + product

    total = times(me, None)
    w[3, 0].wait_recv()
    w[3, 1].wait_recv()
    total = times(sibling, total)

    keys, live = [], []
    for m in range(samples):
        doc_row = doc_v[m : m + 1, :].astype(jnp.float32)
        keys.append(to_column(doc_row) + float(m * seq))
        place = lax.broadcasted_iota(jnp.int32, (seq, 1), 0)
        live.append(jnp.where(place < valid_s[m], 1.0, 0.0))
    key_col = jnp.concatenate(keys, axis=0)
    live_col = jnp.concatenate(live, axis=0)
    key_row = to_row(key_col)
    earlier = jnp.sum(jnp.where(key_row < key_col, 1.0, 0.0), axis=1, keepdims=True)
    order_row = lax.broadcasted_iota(jnp.int32, (rows, rows), 0)
    order_col = lax.broadcasted_iota(jnp.int32, (rows, rows), 1)
    allowed = (key_row == key_col) & (order_col <= order_row)
    offsets = lax.broadcasted_iota(jnp.int32, (rows, 1), 0).astype(jnp.float32) - earlier
    lane = lax.broadcasted_iota(jnp.int32, (1, head), 1)
    half = lax.rem(lane, head // 2).astype(jnp.float32)
    frequency = jnp.exp(half * (-2.0 / head * math.log(ROPE_BASE)))
    angles = offsets * frequency
    cosine = jnp.cos(angles)
    signed = jnp.sin(angles) * jnp.where(lane < head // 2, -1.0, 1.0)

    for part in range(2):
        w[0, part].wait_recv()
        w[2, part] = w_copy(owners[0], part, 2, owners[1])
        w[4, part] = w_copy(owners[0], part, 4, sibling)
        w[1, part].wait_recv()
        w[5, part] = w_copy(owners[1], part, 5, sibling)
    w[1, 2] = w_copy(me, 2, 1, owners[1])

    for place in range(chips):
        crossed[place].wait_recv()
        turned = pl.ds(place * owned, owned)
        dy_turned[turned, :rows] = dy_v[:, block(place * CORES + core, owned)].T
        dy_turned[turned, rows:] = dy_sib[place].T

    total = times(owners[0], total)
    total = times(owners[1], total)

    w[0, 2].wait_recv()
    w[2, 2] = w_copy(owners[0], 2, 2, owners[1])
    w[4, 2] = w_copy(owners[0], 2, 4, sibling)

    mine = block(me, rows)
    columns = {}
    for slot in (2, 0, 1, 6, 5, 4, 3):
        columns[slot] = send(
            x_v.at[:, block(owners[slot], owned)],
            x_all.at[mine],
            a_send_sem.at[slot],
            a_recv_sem.at[slot],
            {"dp": owners[slot]},
        )

    for slot in (4, 5):
        for part in range(2):
            w[slot, part].wait_recv()
        total = times(owners[slot], total)
    for part in range(2):
        w[2, part].wait_recv()
        w[6, part] = w_copy(owners[2], part, 6, sibling)
    w[1, 2].wait_recv()
    w[5, 2] = w_copy(owners[1], 2, 5, sibling)
    total = times(owners[2], total)
    w[2, 2].wait_recv()
    w[6, 2] = w_copy(owners[2], 2, 6, sibling)
    for part in range(2):
        w[6, part].wait_recv()
    projected = times(owners[6], total)

    def turn(vector, sine_part):
        return vector * cosine + pltpu.roll(vector, head // 2, 1) * sine_part

    query = (turn(projected[:, :head], signed) * scale).astype(jnp.bfloat16)
    key = turn(projected[:, head : 2 * head], signed).astype(jnp.bfloat16)
    values = projected[:, 2 * head :].astype(jnp.bfloat16)
    scores = mm(query, key, ((1,), (1,)))
    raised = jnp.where(allowed, jnp.exp(scores), 0.0)
    probs = raised / jnp.sum(raised, axis=1, keepdims=True)
    probs_low = probs.astype(jnp.bfloat16)
    attended = mm(probs_low, values, ((1,), (0,)))
    att[:rows] = (attended * live_col).astype(jnp.bfloat16)
    att_copy = send(
        att.at[:rows],
        att.at[rows:],
        d_send_sem.at[chips],
        d_recv_sem.at[chips],
        {"dp": sibling},
    )

    for slot in (3, 4, 5, 6):
        w[slot, 2].wait_recv()
    d_att = (mm(dy_v[...], wo_all[...], ((1,), (0,))) * live_col).astype(jnp.bfloat16)
    att_copy.wait_recv()

    def out_part(owner):
        return mm(dy_turned[block(owner // CORES, owned), :], att[...], ((1,), (0,)))

    p_copies = []
    for slot in (2, 0, 1):
        p_send[slot] = out_part(owners[slot]).astype(jnp.bfloat16)
        p_copies.append(
            send(
                p_send.at[slot],
                p_recv.at[slot],
                p_send_sem.at[slot],
                p_recv_sem.at[slot],
                {"dp": owners[slot]},
            )
        )

    def y_copy(buf, chunk, owner, slot, device):
        source = buf.at[block(owner, rows)]
        return send(
            source,
            source,
            y_send_sem.at[chunk, slot],
            y_recv_sem.at[chunk, slot],
            {"dp": device},
        )

    d_values = mm(probs_low, d_att, ((0,), (0,)))
    yv_all[mine] = (d_values * inverse).astype(jnp.bfloat16)
    y = {}
    for slot in (2, 0, 1, 3):
        y[0, slot] = y_copy(yv_all, 0, me, slot, owners[slot])
    d_probs = mm(d_att, values, ((1,), (1,)))
    d_scores = (
        probs * (d_probs - jnp.sum(probs * d_probs, axis=1, keepdims=True))
    ).astype(jnp.bfloat16)
    d_query = turn(mm(d_scores, key, ((1,), (0,))) * scale, -signed)
    d_key = turn(mm(d_scores, query, ((0,), (0,))), -signed)
    yqk_all[mine, :head] = (d_query * inverse).astype(jnp.bfloat16)
    yqk_all[mine, head:] = (d_key * inverse).astype(jnp.bfloat16)
    for slot in (2, 0, 1, 3):
        y[1, slot] = y_copy(yqk_all, 1, me, slot, owners[slot])

    out_total = out_part(me)
    x_turned[:, mine] = x_v[:, block(me, owned)].T
    for slot, source in enumerate((0, 1, 2, 3, 5, 4, 6)):
        columns[slot].wait_recv()
        part = block(owners[source], rows)
        x_turned[:, part] = x_all[part].T

    my_piece = pl.ds(pl.multiple_of(rep * piece, 16), piece)

    def z_start(chunk, buf, received, total):
        buf[...] = total.astype(jnp.bfloat16)
        copies = []
        for off in range(1, replicas):
            peer = lax.rem(rep + off, replicas)
            part = pl.ds(pl.multiple_of(peer * piece, 16), piece)
            copies.append(
                send(
                    buf.at[part],
                    received.at[off - 1],
                    r_send_sem.at[chunk, off],
                    r_recv_sem.at[chunk, off],
                    {"rep": peer},
                )
            )
        return copies

    def z_middle(chunk, buf, received, gathered, copies):
        whole = buf[my_piece].astype(jnp.float32)
        for off in range(1, replicas):
            copies[off - 1].wait_recv()
            whole = whole + received[off - 1].astype(jnp.float32)
        gathered[my_piece] = (whole * (1.0 / replicas)).astype(jnp.bfloat16)
        last = []
        for off in range(1, replicas):
            peer = lax.rem(rep + off, replicas)
            last.append(
                send(
                    gathered.at[my_piece],
                    gathered.at[my_piece],
                    g_send_sem.at[chunk, off],
                    g_recv_sem.at[chunk, off],
                    {"rep": peer},
                )
            )
        return last

    def y_pass(buf, chunk):
        for slot, onward in ((0, 4), (1, 5), (2, 6)):
            y[chunk, slot].wait_recv()
            y[chunk, onward] = y_copy(buf, chunk, owners[slot], onward, sibling)

    y_pass(yv_all, 0)
    for slot, copy in zip((2, 0, 1), p_copies):
        copy.wait_recv()
        out_total = out_total + p_recv[slot].astype(jnp.float32)
    out_copies = z_start(0, zg_send, zg_recv, out_total)
    for slot in (3, 4, 5, 6):
        y[0, slot].wait_recv()
    value_total = mm(x_turned[...], yv_all[...], ((1,), (0,)))
    value_copies = z_start(1, zv_send, zv_recv, value_total)
    y_pass(yqk_all, 1)
    for slot in (3, 4, 5, 6):
        y[1, slot].wait_recv()
    both_total = mm(x_turned[...], yqk_all[...], ((1,), (0,)))
    both_copies = z_start(2, zqk_send, zqk_recv, both_total)

    out_last = z_middle(0, zg_send, zg_recv, zg_all, out_copies)
    value_last = z_middle(1, zv_send, zv_recv, zv_all, value_copies)
    both_last = z_middle(2, zqk_send, zqk_recv, zqk_all, both_copies)

    wq_mine = wq_all.at[block(me, owned)]
    for copy in out_last:
        copy.wait_recv()
    go_ref[...] = zg_all[...].astype(jnp.float32)
    for copy in value_last:
        copy.wait_recv()
    value_sum = zv_all[...].astype(jnp.float32)
    gq_ref[:, 2 * head :] = value_sum * gain_col
    gain_sum = value_sum * wq_mine[:, 2 * head :].astype(jnp.float32)
    for copy in both_last:
        copy.wait_recv()
    for place in range(2):
        cols = pl.ds(place * head, head)
        both_sum = zqk_all[:, cols].astype(jnp.float32)
        gq_ref[:, cols] = both_sum * gain_col
        gain_sum = gain_sum + both_sum * wq_mine[:, cols].astype(jnp.float32)
    gg_ref[...] = to_row(jnp.sum(gain_sum, axis=1, keepdims=True))
    for copy in pending:
        copy.wait_send()


def stored(gq_ref, go_ref, gg_ref, gq_out, go_out, gg_out, sem):
    copies = []
    for slot, (source, target) in enumerate(
        ((gq_ref, gq_out), (go_ref, go_out), (gg_ref, gg_out))
    ):
        copy = pltpu.make_async_copy(source, target, sem.at[slot])
        copy.start()
        copies.append(copy)
    for copy in copies:
        copy.wait()


def one_kernel(n, replicas, tokens, cotangent, doc_ids, valid_len, w_qkv, w_out, norm_gain):
    rows, width = tokens.shape
    owned, wide = w_qkv.shape
    head = w_out.shape[1]
    chips = n // CORES
    piece = owned // replicas
    vmem = pl.BlockSpec(memory_space=pltpu.VMEM)
    anywhere = pl.BlockSpec(memory_space=pl.ANY)
    low = jnp.bfloat16
    sem = pltpu.SemaphoreType.DMA
    shapes = (
        jax.ShapeDtypeStruct((owned, wide), jnp.float32),
        jax.ShapeDtypeStruct((owned, head), jnp.float32),
        jax.ShapeDtypeStruct((1, owned), jnp.float32),
    )

    def z_buffers(cols):
        return [
            pltpu.VMEM((owned, cols), low),
            pltpu.VMEM((replicas - 1, piece, cols), low),
            pltpu.VMEM((owned, cols), low),
        ]

    grads = pl.pallas_call(
        functools.partial(fused, n, replicas),
        out_shape=shapes,
        in_specs=[anywhere] * 7,
        out_specs=(vmem, vmem, vmem),
        scratch_shapes=[
            pltpu.VMEM((rows, width), low),
            pltpu.VMEM((rows, width), low),
            pltpu.VMEM(doc_ids.shape, jnp.int32),
            pltpu.SMEM(valid_len.shape, jnp.int32),
            pltpu.VMEM((owned,), low),
            pltpu.VMEM((width, wide), low),
            pltpu.VMEM((width, head), low),
            pltpu.VMEM((n, 8, owned), jnp.float32),
            pltpu.VMEM((rows, width), low),
            pltpu.VMEM((chips, rows, owned), low),
            pltpu.VMEM((chips * owned, CORES * rows), low),
            pltpu.VMEM((CORES * rows, head), low),
            pltpu.VMEM((n * rows, owned), low),
            pltpu.VMEM((owned, n * rows), low),
            pltpu.VMEM((n * rows, head), low),
            pltpu.VMEM((n * rows, 2 * head), low),
            pltpu.VMEM((chips - 1, owned, head), low),
            pltpu.VMEM((chips - 1, owned, head), low),
            *z_buffers(head),
            *z_buffers(head),
            *z_buffers(2 * head),
            sem((7,)),
            sem((n - 1, 3)),
            sem((n - 1, 3)),
            sem((n,)),
            sem((n,)),
            sem((n - 1,)),
            sem((n - 1,)),
            sem((chips + 1,)),
            sem((chips + 1,)),
            sem((chips - 1,)),
            sem((chips - 1,)),
            sem((2, n - 1)),
            sem((2, n - 1)),
            sem((3, replicas)),
            sem((3, replicas)),
            sem((3, replicas)),
            sem((3, replicas)),
        ],
        compiler_params=pltpu.CompilerParams(
            collective_id=0, has_side_effects=True, vmem_limit_bytes=60 * 1024 * 1024
        ),
    )(tokens, cotangent, doc_ids, valid_len, w_qkv, w_out, norm_gain)
    grad_qkv, grad_out, grad_gain = pl.pallas_call(
        stored,
        out_shape=shapes,
        in_specs=[vmem] * 3,
        out_specs=(anywhere,) * 3,
        scratch_shapes=[sem((3,))],
    )(*grads)
    return grad_qkv, grad_out, grad_gain.reshape(owned)


def shards_or_kernel(
    n, replicas, tokens, cotangent, doc_ids, valid_len, w_qkv, w_out, norm_gain
):
    rows, owned, head = tokens.shape[0], w_qkv.shape[0], w_out.shape[1]
    fits = (
        n == 4 * CORES
        and replicas > 1
        and owned % LANES == 0
        and owned % (16 * replicas) == 0
        and rows % LANES == 0
        and rows * n <= 2048
        and head == LANES
        and doc_ids.shape[1] % 8 == 0
    )
    if not fits:
        return shards(tokens, cotangent, doc_ids, valid_len, w_qkv, w_out, norm_gain)
    return one_kernel(
        n, replicas, tokens, cotangent, doc_ids, valid_len, w_qkv, w_out, norm_gain
    )


def solution(mesh):
    in_specs = (
        P(("dp", "rep"), None),
        P(("dp", "rep"), None),
        P(("dp", "rep"), None),
        P(("dp", "rep")),
        P("dp", None),
        P("dp", None),
        P("dp"),
    )
    out_specs = (P("dp", None), P("dp", None), P("dp"))
    body = functools.partial(shards_or_kernel, mesh.shape["dp"], mesh.shape["rep"])
    return jax.shard_map(body, mesh=mesh, in_specs=in_specs, out_specs=out_specs, check_vma=False)
```

```python
import functools
import math

import jax
import jax.numpy as jnp
from jax import lax
from jax.experimental import pallas as pl
from jax.experimental.pallas import tpu as pltpu
from jax.sharding import PartitionSpec as P

NORM_EPS = 1e-06
ROPE_BASE = 1000000.0


def rotate(vector):
    half_size = vector.shape[-1] // 2
    return jnp.concatenate([-vector[..., half_size:], vector[..., :half_size]], axis=-1)


def unrotate(vector):
    half_size = vector.shape[-1] // 2
    return jnp.concatenate([vector[..., half_size:], -vector[..., :half_size]], axis=-1)


def tables(doc_rows, head_size):
    seq_length = doc_rows.shape[1]
    earlier = jnp.sum((doc_rows[:, None, :] < doc_rows[:, :, None]).astype(jnp.int32), axis=2)
    offsets = (jnp.arange(seq_length, dtype=jnp.int32)[None, :] - earlier).astype(jnp.float32)
    frequency = ROPE_BASE ** (-2.0 * jnp.arange(head_size // 2, dtype=jnp.float32) / head_size)
    angles = offsets[:, :, None] * frequency
    angles = jnp.concatenate([angles, angles], axis=2)
    return (jnp.cos(angles), jnp.sin(angles))


def forward_pass(inputs, doc_rows, w_qkv_full, gain_full):
    batches, seq_length, model_width = inputs.shape
    head_size = w_qkv_full.shape[1] // 3
    scale = 1.0 / math.sqrt(head_size)
    wide_in = inputs.astype(jnp.float32)
    inverse_rms = lax.rsqrt(jnp.mean(wide_in * wide_in, axis=2, keepdims=True) + NORM_EPS)
    scaled_in = wide_in * inverse_rms
    normed = (scaled_in * gain_full.astype(jnp.float32)).astype(jnp.bfloat16)
    projected = jnp.dot(
        normed.reshape(-1, model_width), w_qkv_full, preferred_element_type=jnp.float32
    )
    projected = projected.reshape(batches, seq_length, 3 * head_size)
    cosine, sine_part = tables(doc_rows, head_size)
    queries = projected[:, :, :head_size]
    keys_raw = projected[:, :, head_size : 2 * head_size]
    values_raw = projected[:, :, 2 * head_size :]
    query_rot = ((queries * cosine + rotate(queries) * sine_part) * scale).astype(jnp.bfloat16)
    key_rot = (keys_raw * cosine + rotate(keys_raw) * sine_part).astype(jnp.bfloat16)
    values = values_raw.astype(jnp.bfloat16)
    scores = jnp.einsum("msh,mth->mst", query_rot, key_rot, preferred_element_type=jnp.float32)
    order_row = jnp.arange(seq_length, dtype=jnp.int32)[:, None]
    order_col = jnp.arange(seq_length, dtype=jnp.int32)[None, :]
    allowed = (doc_rows[:, :, None] == doc_rows[:, None, :]) & (order_col <= order_row)[None]
    raised = jnp.where(allowed, jnp.exp(scores), 0.0)
    probabilities = raised / jnp.sum(raised, axis=2, keepdims=True)
    probs_low = probabilities.astype(jnp.bfloat16)
    attended = jnp.einsum(
        "mst,mth->msh", probs_low, values, preferred_element_type=jnp.float32
    ).astype(jnp.bfloat16)
    return (
        scaled_in,
        normed,
        query_rot,
        key_rot,
        values,
        probabilities,
        probs_low,
        attended,
        cosine,
        sine_part,
    )


def backward_pass(saved, live_dy, w_qkv_full, w_out_full):
    (
        scaled_in,
        normed,
        query_rot,
        key_rot,
        values,
        probabilities,
        probs_low,
        attended,
        cosine,
        sine_part,
    ) = saved
    batches, seq_length, model_width = live_dy.shape
    head_size = w_out_full.shape[1]
    scale = 1.0 / math.sqrt(head_size)
    d_attended = jnp.dot(
        live_dy.reshape(-1, model_width), w_out_full, preferred_element_type=jnp.float32
    )
    d_attended = d_attended.reshape(batches, seq_length, head_size).astype(jnp.bfloat16)
    d_probs = jnp.einsum("msh,mth->mst", d_attended, values, preferred_element_type=jnp.float32)
    d_values = jnp.einsum("mst,msh->mth", probs_low, d_attended, preferred_element_type=jnp.float32)
    d_scores = (
        probabilities * (d_probs - jnp.sum(probabilities * d_probs, axis=2, keepdims=True))
    ).astype(jnp.bfloat16)
    d_query = (
        jnp.einsum("mst,mth->msh", d_scores, key_rot, preferred_element_type=jnp.float32) * scale
    )
    d_key = jnp.einsum("mst,msh->mth", d_scores, query_rot, preferred_element_type=jnp.float32)
    d_query = d_query * cosine + unrotate(d_query * sine_part)
    d_key = d_key * cosine + unrotate(d_key * sine_part)
    d_qkv = jnp.concatenate([d_query, d_key, d_values], axis=2).astype(jnp.bfloat16)
    d_normed = lax.dot_general(
        d_qkv.reshape(-1, 3 * head_size),
        w_qkv_full,
        (((1,), (1,)), ((), ())),
        preferred_element_type=jnp.float32,
    )
    gain_term = jnp.sum(d_normed * scaled_in.reshape(-1, model_width), axis=0)
    return (d_qkv, gain_term)


def shards(tokens, cotangent, doc_ids, valid_len, w_qkv, w_out, norm_gain):
    batches, seq_length = doc_ids.shape
    model_width = tokens.shape[1]
    inputs = tokens.reshape(batches, seq_length, model_width)
    live_rows = jnp.arange(seq_length, dtype=jnp.int32)[None, :] < valid_len[:, None]
    live_dy = jnp.where(
        live_rows[:, :, None],
        cotangent.reshape(batches, seq_length, model_width),
        jnp.zeros((), jnp.bfloat16),
    )
    full_set = (
        lax.all_gather(w_qkv, "dp", axis=0, tiled=True),
        lax.all_gather(w_out, "dp", axis=0, tiled=True),
        lax.all_gather(norm_gain, "dp", axis=0, tiled=True),
    )
    saved = forward_pass(inputs, doc_ids, full_set[0], full_set[2])
    qkv_all, gain_total = backward_pass(saved, live_dy, full_set[0], full_set[1])
    normed_all = saved[1]
    attended_all = saved[7]
    head_size = w_out.shape[1]
    normed_flat = normed_all.reshape(-1, model_width)
    qkv_flat = qkv_all.reshape(-1, 3 * head_size)
    attended_flat = attended_all.reshape(-1, head_size)
    grad_qkv = lax.dot_general(
        normed_flat, qkv_flat, (((0,), (0,)), ((), ())), preferred_element_type=jnp.float32
    )
    grad_out = lax.dot_general(
        live_dy.reshape(-1, model_width),
        attended_flat,
        (((0,), (0,)), ((), ())),
        preferred_element_type=jnp.float32,
    )
    shares = (
        lax.psum_scatter(grad_qkv, "dp", scatter_dimension=0, tiled=True),
        lax.psum_scatter(grad_out, "dp", scatter_dimension=0, tiled=True),
    )
    shares = lax.psum((shares[0], shares[1]), "rep")
    gain_whole = lax.psum(gain_total, ("dp", "rep"))
    owned_rows = w_qkv.shape[0]
    gain_start = lax.axis_index("dp") * owned_rows
    gain_owned = lax.dynamic_slice_in_dim(gain_whole, gain_start, owned_rows, 0)
    replicas = lax.axis_size("rep")
    return (shares[0] / replicas, shares[1] / replicas, gain_owned / replicas)


MESH = pl.DeviceIdType.MESH
LANES = 128
CORES = 2


def mm(left, right, dims):
    return lax.dot_general(left, right, (dims, ((), ())), preferred_element_type=jnp.float32)


def eye(size):
    return lax.broadcasted_iota(jnp.int32, (size, size), 0) == lax.broadcasted_iota(
        jnp.int32, (size, size), 1
    )


def to_column(row):
    return jnp.sum(jnp.where(eye(row.shape[1]), row, 0.0), axis=1, keepdims=True)


def to_row(column):
    return jnp.sum(jnp.where(eye(column.shape[0]), column, 0.0), axis=0, keepdims=True)


def fused(
    n,
    replicas,
    x_hbm,
    dy_hbm,
    doc_hbm,
    valid_hbm,
    wq_hbm,
    wo_hbm,
    gain_hbm,
    gq_ref,
    go_ref,
    gg_ref,
    x_v,
    dy_v,
    doc_v,
    valid_s,
    gain_v,
    wq_all,
    wo_all,
    gain_all,
    normed,
    dy_sib,
    dy_turned,
    att,
    x_all,
    x_turned,
    y_all,
    p_send,
    p_recv,
    q_send,
    q_recv,
    z_send,
    z_recv,
    z_all,
    in_sem,
    w_send_sem,
    w_recv_sem,
    s_send_sem,
    s_recv_sem,
    a_send_sem,
    a_recv_sem,
    d_send_sem,
    d_recv_sem,
    p_send_sem,
    p_recv_sem,
    q_send_sem,
    q_recv_sem,
    y_send_sem,
    y_recv_sem,
    r_send_sem,
    r_recv_sem,
    g_send_sem,
    g_recv_sem,
):
    me = lax.axis_index("dp")
    rep = lax.axis_index("rep")
    chip, core = me // CORES, lax.rem(me, CORES)
    sibling = chip * CORES + (1 - core)
    rows, width = x_v.shape
    owned = wq_hbm.shape[0]
    head = wo_hbm.shape[1]
    chips = n // CORES
    samples, seq = doc_v.shape
    piece = owned // replicas
    half_owned = owned // 2
    scale = 1.0 / math.sqrt(head)

    def block(index, size):
        return pl.ds(pl.multiple_of(index * size, LANES), size)

    loads = []
    for slot, (source, target) in enumerate(
        (
            (wq_hbm, wq_all.at[block(me, owned)]),
            (wo_hbm, wo_all.at[block(me, owned)]),
            (gain_hbm, gain_v),
            (x_hbm, x_v),
            (dy_hbm, dy_v),
            (doc_hbm, doc_v),
            (valid_hbm, valid_s),
        )
    ):
        load = pltpu.make_async_copy(source, target, in_sem.at[slot])
        load.start()
        loads.append(load)

    barrier = pltpu.get_barrier_semaphore()
    for off in range(1, n):
        pl.semaphore_signal(
            barrier, inc=1, device_id={"dp": lax.rem(me + off, n)}, device_id_type=MESH
        )
    for off in range(1, replicas):
        pl.semaphore_signal(
            barrier,
            inc=1,
            device_id={"rep": lax.rem(rep + off, replicas)},
            device_id_type=MESH,
        )

    pending = []

    def send(src, dst, send_sem, recv_sem, where):
        copy = pltpu.make_async_remote_copy(
            src_ref=src,
            dst_ref=dst,
            send_sem=send_sem,
            recv_sem=recv_sem,
            device_id=where,
            device_id_type=MESH,
        )
        copy.start()
        pending.append(copy)
        return copy

    along, across = lax.rem(chip, 2), chip // 2
    by_x = across * 2 + 1 - along
    by_y = (1 - across) * 2 + along
    first = by_x + core * (by_y - by_x)
    second = by_y + core * (by_x - by_y)
    far = 3 - chip
    owners = (
        first * CORES + core,
        second * CORES + core,
        far * CORES + core,
        sibling,
        second * CORES + 1 - core,
        first * CORES + 1 - core,
        far * CORES + 1 - core,
    )

    def w_part(owner, part):
        if part == 2:
            return wo_all.at[block(owner, owned)]
        start = pl.multiple_of(owner * owned + part * half_owned, LANES)
        return wq_all.at[pl.ds(start, half_owned)]

    def w_copy(owner, part, slot, device):
        source = w_part(owner, part)
        return send(
            source,
            source,
            w_send_sem.at[slot, part],
            w_recv_sem.at[slot, part],
            {"dp": device},
        )

    loads[2].wait()
    gain_row = gain_v[...].reshape(1, owned).astype(jnp.float32)
    gain_all[me] = gain_row
    loads[0].wait()
    loads[1].wait()
    pl.semaphore_wait(barrier, n - 1 + replicas - 1)

    w = {}
    for part in range(2):
        w[0, part] = w_copy(me, part, 0, owners[0])
    for part in range(2):
        w[3, part] = w_copy(me, part, 3, sibling)
    gains = {}
    for off in range(1, n):
        gains[off] = send(
            gain_all.at[me],
            gain_all.at[me],
            s_send_sem.at[off],
            s_recv_sem.at[off],
            {"dp": lax.rem(me + off, n)},
        )
    w[3, 2] = w_copy(me, 2, 3, sibling)

    loads[4].wait()
    crossed = []
    for place in range(chips):
        crossed.append(
            send(
                dy_v.at[:, block(place * CORES + 1 - core, owned)],
                dy_sib.at[place],
                d_send_sem.at[place],
                d_recv_sem.at[place],
                {"dp": sibling},
            )
        )

    loads[3].wait()
    loads[5].wait()
    loads[6].wait()
    gain_col = to_column(gain_row)
    wide_in = x_v[...].astype(jnp.float32)
    inverse = lax.rsqrt(
        jnp.sum(wide_in * wide_in, axis=1, keepdims=True) * (1.0 / width) + NORM_EPS
    )
    keys, live = [], []
    for m in range(samples):
        doc_row = doc_v[m : m + 1, :].astype(jnp.float32)
        keys.append(to_column(doc_row) + float(m * seq))
        place = lax.broadcasted_iota(jnp.int32, (seq, 1), 0)
        live.append(jnp.where(place < valid_s[m], 1.0, 0.0))
    key_col = jnp.concatenate(keys, axis=0)
    live_col = jnp.concatenate(live, axis=0)
    key_row = to_row(key_col)
    earlier = jnp.sum(jnp.where(key_row < key_col, 1.0, 0.0), axis=1, keepdims=True)
    order_row = lax.broadcasted_iota(jnp.int32, (rows, rows), 0)
    order_col = lax.broadcasted_iota(jnp.int32, (rows, rows), 1)
    allowed = (key_row == key_col) & (order_col <= order_row)
    offsets = lax.broadcasted_iota(jnp.int32, (rows, 1), 0).astype(jnp.float32) - earlier
    lane = lax.broadcasted_iota(jnp.int32, (1, head), 1)
    half = lax.rem(lane, head // 2).astype(jnp.float32)
    frequency = jnp.exp(half * (-2.0 / head * math.log(ROPE_BASE)))
    angles = offsets * frequency
    cosine = jnp.cos(angles)
    signed = jnp.sin(angles) * jnp.where(lane < head // 2, -1.0, 1.0)

    for part in range(2):
        w[1, part] = w_copy(me, part, 1, owners[1])
    w[0, 2] = w_copy(me, 2, 0, owners[0])
    for off in range(1, n):
        gains[off].wait_recv()
    for place in range(n):
        cols = pl.ds(place * owned, owned)
        scaled = x_v[:, cols].astype(jnp.float32) * inverse
        normed[:, cols] = (scaled * gain_all[place]).astype(jnp.bfloat16)

    def times(source, total):
        product = mm(normed[:, block(source, owned)], wq_all[block(source, owned), :], ((1,), (0,)))
        return product if total is None else total + product

    total = times(me, None)
    w[3, 0].wait_recv()
    w[3, 1].wait_recv()
    total = times(sibling, total)

    for part in range(2):
        w[0, part].wait_recv()
        w[2, part] = w_copy(owners[0], part, 2, owners[1])
        w[4, part] = w_copy(owners[0], part, 4, sibling)
    w[1, 2] = w_copy(me, 2, 1, owners[1])
    for part in range(2):
        w[1, part].wait_recv()
        w[5, part] = w_copy(owners[1], part, 5, sibling)

    for place in range(chips):
        crossed[place].wait_recv()
        turned = pl.ds(place * owned, owned)
        dy_turned[turned, :rows] = dy_v[:, block(place * CORES + core, owned)].T
        dy_turned[turned, rows:] = dy_sib[place].T

    total = times(owners[0], total)
    total = times(owners[1], total)

    w[0, 2].wait_recv()
    w[2, 2] = w_copy(owners[0], 2, 2, owners[1])
    w[4, 2] = w_copy(owners[0], 2, 4, sibling)

    mine = block(me, rows)
    columns = {}
    for slot in (2, 0, 1, 6, 5, 4, 3):
        columns[slot] = send(
            x_v.at[:, block(owners[slot], owned)],
            x_all.at[mine],
            a_send_sem.at[slot],
            a_recv_sem.at[slot],
            {"dp": owners[slot]},
        )

    for slot in (4, 5):
        for part in range(2):
            w[slot, part].wait_recv()
        total = times(owners[slot], total)
    for part in range(2):
        w[2, part].wait_recv()
        w[6, part] = w_copy(owners[2], part, 6, sibling)
    w[1, 2].wait_recv()
    w[5, 2] = w_copy(owners[1], 2, 5, sibling)
    total = times(owners[2], total)
    w[2, 2].wait_recv()
    w[6, 2] = w_copy(owners[2], 2, 6, sibling)
    for part in range(2):
        w[6, part].wait_recv()
    projected = times(owners[6], total)

    def turn(vector, sine_part):
        return vector * cosine + pltpu.roll(vector, head // 2, 1) * sine_part

    query = (turn(projected[:, :head], signed) * scale).astype(jnp.bfloat16)
    key = turn(projected[:, head : 2 * head], signed).astype(jnp.bfloat16)
    values = projected[:, 2 * head :].astype(jnp.bfloat16)
    scores = mm(query, key, ((1,), (1,)))
    raised = jnp.where(allowed, jnp.exp(scores), 0.0)
    probs = raised / jnp.sum(raised, axis=1, keepdims=True)
    probs_low = probs.astype(jnp.bfloat16)
    attended = mm(probs_low, values, ((1,), (0,)))
    att[:rows] = (attended * live_col).astype(jnp.bfloat16)
    att_copy = send(
        att.at[:rows],
        att.at[rows:],
        d_send_sem.at[chips],
        d_recv_sem.at[chips],
        {"dp": sibling},
    )

    for slot in (3, 4, 5, 6):
        w[slot, 2].wait_recv()
    d_att = (mm(dy_v[...], wo_all[...], ((1,), (0,))) * live_col).astype(jnp.bfloat16)
    att_copy.wait_recv()

    by_chip = mm(dy_turned[...], att[...], ((1,), (0,)))
    p_send[...] = by_chip.reshape(chips, replicas, piece, head).astype(jnp.bfloat16)
    p_copies = []
    for off in range(1, replicas):
        peer = lax.rem(rep + off, replicas)
        p_copies.append(
            send(
                p_send.at[:, peer],
                p_recv.at[off - 1],
                p_send_sem.at[off],
                p_recv_sem.at[off],
                {"rep": peer},
            )
        )

    y = {}

    def y_copy(chunk, owner, slot, device):
        source = y_all.at[chunk].at[block(owner, rows)]
        y[chunk, slot] = send(
            source,
            source,
            y_send_sem.at[chunk, slot],
            y_recv_sem.at[chunk, slot],
            {"dp": device},
        )

    def y_start(chunk, value):
        y_all[chunk, mine] = (value * inverse).astype(jnp.bfloat16)
        for slot in (2, 0, 1, 3):
            y_copy(chunk, me, slot, owners[slot])

    y_start(0, mm(probs_low, d_att, ((0,), (0,))))
    d_probs = mm(d_att, values, ((1,), (1,)))
    d_scores = (
        probs * (d_probs - jnp.sum(probs * d_probs, axis=1, keepdims=True))
    ).astype(jnp.bfloat16)
    y_start(1, turn(mm(d_scores, key, ((1,), (0,))) * scale, -signed))
    y_start(2, turn(mm(d_scores, query, ((0,), (0,))), -signed))

    x_turned[:, mine] = x_v[:, block(me, owned)].T
    for slot, source in enumerate((0, 1, 2, 3, 5, 4, 6)):
        columns[slot].wait_recv()
        part = block(owners[source], rows)
        x_turned[:, part] = x_all[part].T

    my_piece = pl.ds(pl.multiple_of(rep * piece, 16), piece)
    r, g = {}, {}

    def y_pass(chunk):
        for slot, onward in ((2, 6), (0, 4), (1, 5)):
            y[chunk, slot].wait_recv()
            y_copy(chunk, owners[slot], onward, sibling)

    def y_finish(chunk):
        for slot in (3, 4, 5, 6):
            y[chunk, slot].wait_recv()
        total = mm(x_turned[...], y_all[chunk], ((1,), (0,)))
        z_send[chunk] = total.astype(jnp.bfloat16)
        for off in range(1, replicas):
            peer = lax.rem(rep + off, replicas)
            part = pl.ds(pl.multiple_of(peer * piece, 16), piece)
            r[chunk, off] = send(
                z_send.at[chunk].at[part],
                z_recv.at[chunk, off - 1],
                r_send_sem.at[chunk, off],
                r_recv_sem.at[chunk, off],
                {"rep": peer},
            )

    def z_gather(chunk, whole):
        z_all[chunk, my_piece] = (whole * (1.0 / replicas)).astype(jnp.bfloat16)
        for off in range(1, replicas):
            g[chunk, off] = send(
                z_all.at[chunk].at[my_piece],
                z_all.at[chunk].at[my_piece],
                g_send_sem.at[chunk, off],
                g_recv_sem.at[chunk, off],
                {"rep": lax.rem(rep + off, replicas)},
            )

    def z_sum(chunk):
        whole = z_send[chunk, my_piece].astype(jnp.float32)
        for off in range(1, replicas):
            r[chunk, off].wait_recv()
            whole = whole + z_recv[chunk, off - 1].astype(jnp.float32)
        z_gather(chunk, whole)

    y_pass(0)
    y_finish(0)
    y_pass(1)
    q_whole = p_send[:, rep].astype(jnp.float32)
    for off in range(1, replicas):
        p_copies[off - 1].wait_recv()
        q_whole = q_whole + p_recv[off - 1].astype(jnp.float32)
    q_send[...] = q_whole.astype(jnp.bfloat16)
    q_copies = []
    for slot in range(chips - 1):
        q_copies.append(
            send(
                q_send.at[owners[slot] // CORES],
                q_recv.at[slot],
                q_send_sem.at[slot],
                q_recv_sem.at[slot],
                {"dp": owners[slot]},
            )
        )
    y_finish(1)
    y_pass(2)
    y_finish(2)
    whole = q_send[chip].astype(jnp.float32)
    for slot in range(chips - 1):
        q_copies[slot].wait_recv()
        whole = whole + q_recv[slot].astype(jnp.float32)
    z_gather(3, whole)
    z_sum(0)
    z_sum(1)
    z_sum(2)

    def gathered(chunk):
        for off in range(1, replicas):
            g[chunk, off].wait_recv()
        return z_all[chunk].astype(jnp.float32)

    go_ref[...] = gathered(3)
    wq_mine = wq_all.at[block(me, owned)]
    gain_sum = jnp.zeros((owned, head), jnp.float32)
    for chunk, place in ((0, 2), (1, 0), (2, 1)):
        cols = pl.ds(place * head, head)
        summed = gathered(chunk)
        gq_ref[:, cols] = summed * gain_col
        gain_sum = gain_sum + summed * wq_mine[:, cols].astype(jnp.float32)
    gg_ref[...] = to_row(jnp.sum(gain_sum, axis=1, keepdims=True))
    for copy in pending:
        copy.wait_send()


def stored(gq_ref, go_ref, gg_ref, gq_out, go_out, gg_out, sem):
    copies = []
    for slot, (source, target) in enumerate(
        ((gq_ref, gq_out), (go_ref, go_out), (gg_ref, gg_out))
    ):
        copy = pltpu.make_async_copy(source, target, sem.at[slot])
        copy.start()
        copies.append(copy)
    for copy in copies:
        copy.wait()


def one_kernel(n, replicas, tokens, cotangent, doc_ids, valid_len, w_qkv, w_out, norm_gain):
    rows, width = tokens.shape
    owned, wide = w_qkv.shape
    head = w_out.shape[1]
    chips = n // CORES
    piece = owned // replicas
    vmem = pl.BlockSpec(memory_space=pltpu.VMEM)
    hbm = pl.BlockSpec(memory_space=pltpu.HBM)
    low = jnp.bfloat16
    sem = pltpu.SemaphoreType.DMA
    shapes = (
        jax.ShapeDtypeStruct((owned, wide), jnp.float32),
        jax.ShapeDtypeStruct((owned, head), jnp.float32),
        jax.ShapeDtypeStruct((1, owned), jnp.float32),
    )

    grads = pl.pallas_call(
        functools.partial(fused, n, replicas),
        out_shape=shapes,
        in_specs=[hbm] * 7,
        out_specs=(vmem, vmem, vmem),
        scratch_shapes=[
            pltpu.VMEM((rows, width), low),
            pltpu.VMEM((rows, width), low),
            pltpu.VMEM(doc_ids.shape, jnp.int32),
            pltpu.SMEM(valid_len.shape, jnp.int32),
            pltpu.VMEM((owned,), low),
            pltpu.VMEM((width, wide), low),
            pltpu.VMEM((width, head), low),
            pltpu.VMEM((n, 1, owned), jnp.float32),
            pltpu.VMEM((rows, width), low),
            pltpu.VMEM((chips, rows, owned), low),
            pltpu.VMEM((chips * owned, CORES * rows), low),
            pltpu.VMEM((CORES * rows, head), low),
            pltpu.VMEM((n * rows, owned), low),
            pltpu.VMEM((owned, n * rows), low),
            pltpu.VMEM((3, n * rows, head), low),
            pltpu.VMEM((chips, replicas, piece, head), low),
            pltpu.VMEM((replicas - 1, chips, piece, head), low),
            pltpu.VMEM((chips, piece, head), low),
            pltpu.VMEM((chips - 1, piece, head), low),
            pltpu.VMEM((3, owned, head), low),
            pltpu.VMEM((3, replicas - 1, piece, head), low),
            pltpu.VMEM((4, owned, head), low),
            sem((7,)),
            sem((n - 1, 3)),
            sem((n - 1, 3)),
            sem((n,)),
            sem((n,)),
            sem((n - 1,)),
            sem((n - 1,)),
            sem((chips + 1,)),
            sem((chips + 1,)),
            sem((replicas,)),
            sem((replicas,)),
            sem((chips - 1,)),
            sem((chips - 1,)),
            sem((3, n - 1)),
            sem((3, n - 1)),
            sem((3, replicas)),
            sem((3, replicas)),
            sem((4, replicas)),
            sem((4, replicas)),
        ],
        compiler_params=pltpu.CompilerParams(
            collective_id=0, has_side_effects=True, vmem_limit_bytes=32 * 1024 * 1024
        ),
    )(
        *(
            pltpu.with_memory_space_constraint(array, pltpu.HBM)
            for array in (tokens, cotangent, doc_ids, valid_len, w_qkv, w_out, norm_gain)
        )
    )
    grad_qkv, grad_out, grad_gain = pl.pallas_call(
        stored,
        out_shape=shapes,
        in_specs=[vmem] * 3,
        out_specs=(hbm,) * 3,
        scratch_shapes=[sem((3,))],
        compiler_params=pltpu.CompilerParams(vmem_limit_bytes=4 * 1024 * 1024),
    )(*grads)
    return grad_qkv, grad_out, grad_gain.reshape(owned)


def shards_or_kernel(
    n, replicas, tokens, cotangent, doc_ids, valid_len, w_qkv, w_out, norm_gain
):
    rows, owned, head = tokens.shape[0], w_qkv.shape[0], w_out.shape[1]
    fits = (
        n == 4 * CORES
        and replicas > 1
        and owned % LANES == 0
        and owned % (16 * replicas) == 0
        and rows % LANES == 0
        and rows * n <= 2048
        and head == LANES
        and doc_ids.shape[1] % 8 == 0
    )
    if not fits:
        return shards(tokens, cotangent, doc_ids, valid_len, w_qkv, w_out, norm_gain)
    return one_kernel(
        n, replicas, tokens, cotangent, doc_ids, valid_len, w_qkv, w_out, norm_gain
    )


def solution(mesh):
    in_specs = (
        P(("dp", "rep"), None),
        P(("dp", "rep"), None),
        P(("dp", "rep"), None),
        P(("dp", "rep")),
        P("dp", None),
        P("dp", None),
        P("dp"),
    )
    out_specs = (P("dp", None), P("dp", None), P("dp"))
    body = functools.partial(shards_or_kernel, mesh.shape["dp"], mesh.shape["rep"])
    return jax.shard_map(body, mesh=mesh, in_specs=in_specs, out_specs=out_specs, check_vma=False)
```

```python
import functools
import math

import jax
import jax.numpy as jnp
from jax import lax
from jax.experimental import pallas as pl
from jax.experimental.pallas import tpu as pltpu
from jax.sharding import PartitionSpec as P

NORM_EPS = 1e-06
ROPE_BASE = 1000000.0


def rotate(vector):
    half_size = vector.shape[-1] // 2
    return jnp.concatenate([-vector[..., half_size:], vector[..., :half_size]], axis=-1)


def unrotate(vector):
    half_size = vector.shape[-1] // 2
    return jnp.concatenate([vector[..., half_size:], -vector[..., :half_size]], axis=-1)


def tables(doc_rows, head_size):
    seq_length = doc_rows.shape[1]
    earlier = jnp.sum((doc_rows[:, None, :] < doc_rows[:, :, None]).astype(jnp.int32), axis=2)
    offsets = (jnp.arange(seq_length, dtype=jnp.int32)[None, :] - earlier).astype(jnp.float32)
    frequency = ROPE_BASE ** (-2.0 * jnp.arange(head_size // 2, dtype=jnp.float32) / head_size)
    angles = offsets[:, :, None] * frequency
    angles = jnp.concatenate([angles, angles], axis=2)
    return (jnp.cos(angles), jnp.sin(angles))


def forward_pass(inputs, doc_rows, w_qkv_full, gain_full):
    batches, seq_length, model_width = inputs.shape
    head_size = w_qkv_full.shape[1] // 3
    scale = 1.0 / math.sqrt(head_size)
    wide_in = inputs.astype(jnp.float32)
    inverse_rms = lax.rsqrt(jnp.mean(wide_in * wide_in, axis=2, keepdims=True) + NORM_EPS)
    scaled_in = wide_in * inverse_rms
    normed = (scaled_in * gain_full.astype(jnp.float32)).astype(jnp.bfloat16)
    projected = jnp.dot(
        normed.reshape(-1, model_width), w_qkv_full, preferred_element_type=jnp.float32
    )
    projected = projected.reshape(batches, seq_length, 3 * head_size)
    cosine, sine_part = tables(doc_rows, head_size)
    queries = projected[:, :, :head_size]
    keys_raw = projected[:, :, head_size : 2 * head_size]
    values_raw = projected[:, :, 2 * head_size :]
    query_rot = ((queries * cosine + rotate(queries) * sine_part) * scale).astype(jnp.bfloat16)
    key_rot = (keys_raw * cosine + rotate(keys_raw) * sine_part).astype(jnp.bfloat16)
    values = values_raw.astype(jnp.bfloat16)
    scores = jnp.einsum("msh,mth->mst", query_rot, key_rot, preferred_element_type=jnp.float32)
    order_row = jnp.arange(seq_length, dtype=jnp.int32)[:, None]
    order_col = jnp.arange(seq_length, dtype=jnp.int32)[None, :]
    allowed = (doc_rows[:, :, None] == doc_rows[:, None, :]) & (order_col <= order_row)[None]
    raised = jnp.where(allowed, jnp.exp(scores), 0.0)
    probabilities = raised / jnp.sum(raised, axis=2, keepdims=True)
    probs_low = probabilities.astype(jnp.bfloat16)
    attended = jnp.einsum(
        "mst,mth->msh", probs_low, values, preferred_element_type=jnp.float32
    ).astype(jnp.bfloat16)
    return (
        scaled_in,
        normed,
        query_rot,
        key_rot,
        values,
        probabilities,
        probs_low,
        attended,
        cosine,
        sine_part,
    )


def backward_pass(saved, live_dy, w_qkv_full, w_out_full):
    (
        scaled_in,
        normed,
        query_rot,
        key_rot,
        values,
        probabilities,
        probs_low,
        attended,
        cosine,
        sine_part,
    ) = saved
    batches, seq_length, model_width = live_dy.shape
    head_size = w_out_full.shape[1]
    scale = 1.0 / math.sqrt(head_size)
    d_attended = jnp.dot(
        live_dy.reshape(-1, model_width), w_out_full, preferred_element_type=jnp.float32
    )
    d_attended = d_attended.reshape(batches, seq_length, head_size).astype(jnp.bfloat16)
    d_probs = jnp.einsum("msh,mth->mst", d_attended, values, preferred_element_type=jnp.float32)
    d_values = jnp.einsum("mst,msh->mth", probs_low, d_attended, preferred_element_type=jnp.float32)
    d_scores = (
        probabilities * (d_probs - jnp.sum(probabilities * d_probs, axis=2, keepdims=True))
    ).astype(jnp.bfloat16)
    d_query = (
        jnp.einsum("mst,mth->msh", d_scores, key_rot, preferred_element_type=jnp.float32) * scale
    )
    d_key = jnp.einsum("mst,msh->mth", d_scores, query_rot, preferred_element_type=jnp.float32)
    d_query = d_query * cosine + unrotate(d_query * sine_part)
    d_key = d_key * cosine + unrotate(d_key * sine_part)
    d_qkv = jnp.concatenate([d_query, d_key, d_values], axis=2).astype(jnp.bfloat16)
    d_normed = lax.dot_general(
        d_qkv.reshape(-1, 3 * head_size),
        w_qkv_full,
        (((1,), (1,)), ((), ())),
        preferred_element_type=jnp.float32,
    )
    gain_term = jnp.sum(d_normed * scaled_in.reshape(-1, model_width), axis=0)
    return (d_qkv, gain_term)


def shards(tokens, cotangent, doc_ids, valid_len, w_qkv, w_out, norm_gain):
    batches, seq_length = doc_ids.shape
    model_width = tokens.shape[1]
    inputs = tokens.reshape(batches, seq_length, model_width)
    live_rows = jnp.arange(seq_length, dtype=jnp.int32)[None, :] < valid_len[:, None]
    live_dy = jnp.where(
        live_rows[:, :, None],
        cotangent.reshape(batches, seq_length, model_width),
        jnp.zeros((), jnp.bfloat16),
    )
    full_set = (
        lax.all_gather(w_qkv, "dp", axis=0, tiled=True),
        lax.all_gather(w_out, "dp", axis=0, tiled=True),
        lax.all_gather(norm_gain, "dp", axis=0, tiled=True),
    )
    saved = forward_pass(inputs, doc_ids, full_set[0], full_set[2])
    qkv_all, gain_total = backward_pass(saved, live_dy, full_set[0], full_set[1])
    normed_all = saved[1]
    attended_all = saved[7]
    head_size = w_out.shape[1]
    normed_flat = normed_all.reshape(-1, model_width)
    qkv_flat = qkv_all.reshape(-1, 3 * head_size)
    attended_flat = attended_all.reshape(-1, head_size)
    grad_qkv = lax.dot_general(
        normed_flat, qkv_flat, (((0,), (0,)), ((), ())), preferred_element_type=jnp.float32
    )
    grad_out = lax.dot_general(
        live_dy.reshape(-1, model_width),
        attended_flat,
        (((0,), (0,)), ((), ())),
        preferred_element_type=jnp.float32,
    )
    shares = (
        lax.psum_scatter(grad_qkv, "dp", scatter_dimension=0, tiled=True),
        lax.psum_scatter(grad_out, "dp", scatter_dimension=0, tiled=True),
    )
    shares = lax.psum((shares[0], shares[1]), "rep")
    gain_whole = lax.psum(gain_total, ("dp", "rep"))
    owned_rows = w_qkv.shape[0]
    gain_start = lax.axis_index("dp") * owned_rows
    gain_owned = lax.dynamic_slice_in_dim(gain_whole, gain_start, owned_rows, 0)
    replicas = lax.axis_size("rep")
    return (shares[0] / replicas, shares[1] / replicas, gain_owned / replicas)


MESH = pl.DeviceIdType.MESH
LANES = 128
CORES = 2


def mm(left, right, dims):
    return lax.dot_general(left, right, (dims, ((), ())), preferred_element_type=jnp.float32)


def eye(size):
    return lax.broadcasted_iota(jnp.int32, (size, size), 0) == lax.broadcasted_iota(
        jnp.int32, (size, size), 1
    )


def to_column(row):
    return jnp.sum(jnp.where(eye(row.shape[1]), row, 0.0), axis=1, keepdims=True)


def to_row(column):
    return jnp.sum(jnp.where(eye(column.shape[0]), column, 0.0), axis=0, keepdims=True)


def fused(
    n,
    replicas,
    x_hbm,
    dy_hbm,
    doc_hbm,
    valid_hbm,
    wq_hbm,
    wo_hbm,
    gain_hbm,
    gq_ref,
    go_ref,
    gg_ref,
    x_v,
    dy_v,
    doc_v,
    valid_s,
    gain_v,
    wq_all,
    wo_all,
    gain_all,
    normed,
    dy_sib,
    dy_turned,
    att,
    x_all,
    x_turned,
    y_all,
    p_send,
    p_recv,
    q_send,
    q_recv,
    z_send,
    z_recv,
    z_all,
    in_sem,
    w_send_sem,
    w_recv_sem,
    s_send_sem,
    s_recv_sem,
    a_send_sem,
    a_recv_sem,
    d_send_sem,
    d_recv_sem,
    p_send_sem,
    p_recv_sem,
    q_send_sem,
    q_recv_sem,
    y_send_sem,
    y_recv_sem,
    r_send_sem,
    r_recv_sem,
    g_send_sem,
    g_recv_sem,
):
    me = lax.axis_index("dp")
    rep = lax.axis_index("rep")
    chip, core = me // CORES, lax.rem(me, CORES)
    sibling = chip * CORES + (1 - core)
    rows, width = x_v.shape
    owned = wq_hbm.shape[0]
    head = wo_hbm.shape[1]
    chips = n // CORES
    samples, seq = doc_v.shape
    piece = owned // replicas
    half_owned = owned // 2
    scale = 1.0 / math.sqrt(head)

    def block(index, size):
        return pl.ds(pl.multiple_of(index * size, LANES), size)

    loads = []
    for slot, (source, target) in enumerate(
        (
            (wq_hbm, wq_all.at[block(me, owned)]),
            (wo_hbm, wo_all.at[block(me, owned)]),
            (gain_hbm, gain_v),
            (x_hbm, x_v),
            (dy_hbm, dy_v),
            (doc_hbm, doc_v),
            (valid_hbm, valid_s),
        )
    ):
        load = pltpu.make_async_copy(source, target, in_sem.at[slot])
        load.start()
        loads.append(load)

    barrier = pltpu.get_barrier_semaphore()
    for off in range(1, n):
        pl.semaphore_signal(
            barrier, inc=1, device_id={"dp": lax.rem(me + off, n)}, device_id_type=MESH
        )
    for off in range(1, replicas):
        pl.semaphore_signal(
            barrier,
            inc=1,
            device_id={"rep": lax.rem(rep + off, replicas)},
            device_id_type=MESH,
        )

    pending = []

    def send(src, dst, send_sem, recv_sem, where):
        copy = pltpu.make_async_remote_copy(
            src_ref=src,
            dst_ref=dst,
            send_sem=send_sem,
            recv_sem=recv_sem,
            device_id=where,
            device_id_type=MESH,
        )
        copy.start()
        pending.append(copy)
        return copy

    along, across = lax.rem(chip, 2), chip // 2
    by_x = across * 2 + 1 - along
    by_y = (1 - across) * 2 + along
    first = by_x + core * (by_y - by_x)
    second = by_y + core * (by_x - by_y)
    far = 3 - chip
    owners = (
        first * CORES + core,
        second * CORES + core,
        far * CORES + core,
        sibling,
        second * CORES + 1 - core,
        first * CORES + 1 - core,
        far * CORES + 1 - core,
    )

    def w_part(owner, part):
        if part == 2:
            return wo_all.at[block(owner, owned)]
        start = pl.multiple_of(owner * owned + part * half_owned, LANES)
        return wq_all.at[pl.ds(start, half_owned)]

    def w_copy(owner, part, slot, device):
        source = w_part(owner, part)
        return send(
            source,
            source,
            w_send_sem.at[slot, part],
            w_recv_sem.at[slot, part],
            {"dp": device},
        )

    side = lax.rem(rep, 2)
    partner = rep + 1 - 2 * side

    def w_half(owner, part, which):
        start = pl.multiple_of(owner * owned + which * half_owned, LANES)
        return (wo_all if part == 2 else wq_all).at[pl.ds(start, half_owned)]

    def half_copy(owner, part, which, slot, where):
        source = w_half(owner, part, which)
        return send(source, source, w_send_sem.at[slot, part], w_recv_sem.at[slot, part], where)

    loads[2].wait()
    gain_row = gain_v[...].reshape(1, owned).astype(jnp.float32)
    gain_all[me] = gain_row
    loads[0].wait()
    loads[1].wait()
    pl.semaphore_wait(barrier, n - 1 + replicas - 1)

    gains = {}
    for off in range(1, n):
        gains[off] = send(
            gain_all.at[me],
            gain_all.at[me],
            s_send_sem.at[off],
            s_recv_sem.at[off],
            {"dp": lax.rem(me + off, n)},
        )
    w = {}
    for part in range(2):
        w[0, part] = w_copy(me, part, 0, owners[0])
    for part in range(2):
        w[3, part] = w_copy(me, part, 3, sibling)
    w[3, 2] = w_copy(me, 2, 3, sibling)

    loads[4].wait()
    crossed = []
    for place in range(chips):
        crossed.append(
            send(
                dy_v.at[:, block(place * CORES + 1 - core, owned)],
                dy_sib.at[place],
                d_send_sem.at[place],
                d_recv_sem.at[place],
                {"dp": sibling},
            )
        )

    loads[3].wait()
    loads[5].wait()
    loads[6].wait()
    gain_col = to_column(gain_row)
    wide_in = x_v[...].astype(jnp.float32)
    inverse = lax.rsqrt(
        jnp.sum(wide_in * wide_in, axis=1, keepdims=True) * (1.0 / width) + NORM_EPS
    )
    keys, live = [], []
    for m in range(samples):
        doc_row = doc_v[m : m + 1, :].astype(jnp.float32)
        keys.append(to_column(doc_row) + float(m * seq))
        place = lax.broadcasted_iota(jnp.int32, (seq, 1), 0)
        live.append(jnp.where(place < valid_s[m], 1.0, 0.0))
    key_col = jnp.concatenate(keys, axis=0)
    live_col = jnp.concatenate(live, axis=0)
    key_row = to_row(key_col)
    earlier = jnp.sum(jnp.where(key_row < key_col, 1.0, 0.0), axis=1, keepdims=True)
    order_row = lax.broadcasted_iota(jnp.int32, (rows, rows), 0)
    order_col = lax.broadcasted_iota(jnp.int32, (rows, rows), 1)
    allowed = (key_row == key_col) & (order_col <= order_row)
    offsets = lax.broadcasted_iota(jnp.int32, (rows, 1), 0).astype(jnp.float32) - earlier
    lane = lax.broadcasted_iota(jnp.int32, (1, head), 1)
    half = lax.rem(lane, head // 2).astype(jnp.float32)
    frequency = jnp.exp(half * (-2.0 / head * math.log(ROPE_BASE)))
    angles = offsets * frequency
    cosine = jnp.cos(angles)
    signed = jnp.sin(angles) * jnp.where(lane < head // 2, -1.0, 1.0)

    for part in (0, 2):
        w[1, part] = half_copy(me, part, side, 1, {"dp": owners[1]})
    w[0, 2] = w_copy(me, 2, 0, owners[0])
    mine = block(me, rows)
    columns = {}

    def x_copy(slot):
        columns[slot] = send(
            x_v.at[:, block(owners[slot], owned)],
            x_all.at[mine],
            a_send_sem.at[slot],
            a_recv_sem.at[slot],
            {"dp": owners[slot]},
        )

    for slot in (3,0,5,1):
        x_copy(slot)
    for off in range(1, n):
        gains[off].wait_recv()
    for place in range(n):
        cols = pl.ds(place * owned, owned)
        scaled = x_v[:, cols].astype(jnp.float32) * inverse
        normed[:, cols] = (scaled * gain_all[place]).astype(jnp.bfloat16)

    def times(source, total):
        product = mm(normed[:, block(source, owned)], wq_all[block(source, owned), :], ((1,), (0,)))
        return product if total is None else total + product

    total = times(me, None)
    w[3, 0].wait_recv()
    w[3, 1].wait_recv()
    total = times(sibling, total)

    for part in range(2):
        w[0, part].wait_recv()
        w[2, part] = w_copy(owners[0], part, 2, owners[1])
        w[4, part] = w_copy(owners[0], part, 4, sibling)
    for part in (0, 2):
        w[1, part].wait_recv()
        w[7, part] = half_copy(owners[1], part, side, 7, {"rep": partner})
        w[5, part] = half_copy(owners[1], part, side, 5, {"dp": sibling})

    for place in range(chips):
        crossed[place].wait_recv()
        turned = pl.ds(place * owned, owned)
        dy_turned[turned, :rows] = dy_v[:, block(place * CORES + core, owned)].T
        dy_turned[turned, rows:] = dy_sib[place].T

    total = times(owners[0], total)

    w[0, 2].wait_recv()
    w[2, 2] = w_copy(owners[0], 2, 2, owners[1])
    w[4, 2] = w_copy(owners[0], 2, 4, sibling)
    for slot in (2,6,4):
        x_copy(slot)

    for part in range(2):
        w[4, part].wait_recv()
    total = times(owners[4], total)
    for part in range(2):
        w[2, part].wait_recv()
        w[6, part] = w_copy(owners[2], part, 6, sibling)
    for part in (0, 2):
        w[7, part].wait_recv()
        w[8, part] = half_copy(owners[1], part, 1 - side, 8, {"dp": sibling})

    total = times(owners[1], total)
    total = times(owners[2], total)
    w[2, 2].wait_recv()
    w[6, 2] = w_copy(owners[2], 2, 6, sibling)
    w[5, 0].wait_recv()
    w[8, 0].wait_recv()
    total = times(owners[5], total)
    for part in range(2):
        w[6, part].wait_recv()
    projected = times(owners[6], total)

    def turn(vector, sine_part):
        return vector * cosine + pltpu.roll(vector, head // 2, 1) * sine_part

    query = (turn(projected[:, :head], signed) * scale).astype(jnp.bfloat16)
    key = turn(projected[:, head : 2 * head], signed).astype(jnp.bfloat16)
    values = projected[:, 2 * head :].astype(jnp.bfloat16)
    scores = mm(query, key, ((1,), (1,)))
    raised = jnp.where(allowed, jnp.exp(scores), 0.0)
    probs = raised / jnp.sum(raised, axis=1, keepdims=True)
    probs_low = probs.astype(jnp.bfloat16)
    attended = mm(probs_low, values, ((1,), (0,)))
    att[:rows] = (attended * live_col).astype(jnp.bfloat16)
    att_copy = send(
        att.at[:rows],
        att.at[rows:],
        d_send_sem.at[chips],
        d_recv_sem.at[chips],
        {"dp": sibling},
    )

    for slot in (3, 4, 5, 8, 6):
        w[slot, 2].wait_recv()
    d_att = (mm(dy_v[...], wo_all[...], ((1,), (0,))) * live_col).astype(jnp.bfloat16)
    att_copy.wait_recv()

    by_chip = mm(dy_turned[...], att[...], ((1,), (0,)))
    p_send[...] = by_chip.reshape(chips, replicas, piece, head).astype(jnp.bfloat16)
    p_copies = []
    for off in range(1, replicas):
        peer = lax.rem(rep + off, replicas)
        p_copies.append(
            send(
                p_send.at[:, peer],
                p_recv.at[off - 1],
                p_send_sem.at[off],
                p_recv_sem.at[off],
                {"rep": peer},
            )
        )

    y = {}

    def y_copy(chunk, owner, slot, device):
        source = y_all.at[chunk].at[block(owner, rows)]
        y[chunk, slot] = send(
            source,
            source,
            y_send_sem.at[chunk, slot],
            y_recv_sem.at[chunk, slot],
            {"dp": device},
        )

    def y_start(chunk, value):
        y_all[chunk, mine] = (value * inverse).astype(jnp.bfloat16)
        for slot in (2, 0, 1, 3):
            y_copy(chunk, me, slot, owners[slot])

    y_start(0, mm(probs_low, d_att, ((0,), (0,))))
    d_probs = mm(d_att, values, ((1,), (1,)))
    d_scores = (
        probs * (d_probs - jnp.sum(probs * d_probs, axis=1, keepdims=True))
    ).astype(jnp.bfloat16)
    y_start(1, turn(mm(d_scores, key, ((1,), (0,))) * scale, -signed))
    y_start(2, turn(mm(d_scores, query, ((0,), (0,))), -signed))

    x_turned[:, mine] = x_v[:, block(me, owned)].T
    for slot, source in enumerate((0, 1, 2, 3, 5, 4, 6)):
        columns[slot].wait_recv()
        part = block(owners[source], rows)
        x_turned[:, part] = x_all[part].T

    my_piece = pl.ds(pl.multiple_of(rep * piece, 16), piece)
    r, g = {}, {}

    def y_pass(chunk):
        for slot, onward in ((2, 6), (0, 4), (1, 5)):
            y[chunk, slot].wait_recv()
            y_copy(chunk, owners[slot], onward, sibling)

    def y_finish(chunk):
        for slot in (3, 4, 5, 6):
            y[chunk, slot].wait_recv()
        total = mm(x_turned[...], y_all[chunk], ((1,), (0,)))
        z_send[chunk] = total.astype(jnp.bfloat16)
        for off in range(1, replicas):
            peer = lax.rem(rep + off, replicas)
            part = pl.ds(pl.multiple_of(peer * piece, 16), piece)
            r[chunk, off] = send(
                z_send.at[chunk].at[part],
                z_recv.at[chunk, off - 1],
                r_send_sem.at[chunk, off],
                r_recv_sem.at[chunk, off],
                {"rep": peer},
            )

    def z_gather(chunk, whole):
        z_all[chunk, my_piece] = (whole * (1.0 / replicas)).astype(jnp.bfloat16)
        for off in range(1, replicas):
            g[chunk, off] = send(
                z_all.at[chunk].at[my_piece],
                z_all.at[chunk].at[my_piece],
                g_send_sem.at[chunk, off],
                g_recv_sem.at[chunk, off],
                {"rep": lax.rem(rep + off, replicas)},
            )

    def z_sum(chunk):
        whole = z_send[chunk, my_piece].astype(jnp.float32)
        for off in range(1, replicas):
            r[chunk, off].wait_recv()
            whole = whole + z_recv[chunk, off - 1].astype(jnp.float32)
        z_gather(chunk, whole)

    y_pass(0)
    y_pass(1)
    y_finish(0)
    y_pass(2)
    y_finish(1)
    y_finish(2)
    q_whole = p_send[:, rep].astype(jnp.float32)
    for off in range(1, replicas):
        p_copies[off - 1].wait_recv()
        q_whole = q_whole + p_recv[off - 1].astype(jnp.float32)
    q_send[...] = q_whole.astype(jnp.bfloat16)
    q_copies = []
    for slot in range(chips - 1):
        q_copies.append(
            send(
                q_send.at[owners[slot] // CORES],
                q_recv.at[slot],
                q_send_sem.at[slot],
                q_recv_sem.at[slot],
                {"dp": owners[slot]},
            )
        )
    z_sum(0)
    z_sum(1)
    whole = q_send[chip].astype(jnp.float32)
    for slot in range(chips - 1):
        q_copies[slot].wait_recv()
        whole = whole + q_recv[slot].astype(jnp.float32)
    z_gather(3, whole)
    z_sum(2)

    def gathered(chunk):
        for off in range(1, replicas):
            g[chunk, off].wait_recv()
        return z_all[chunk].astype(jnp.float32)

    wq_mine = wq_all.at[block(me, owned)]
    gain_sum = jnp.zeros((owned, head), jnp.float32)
    for chunk, place in ((0, 2), (1, 0), (2, 1)):
        cols = pl.ds(place * head, head)
        summed = gathered(chunk)
        gq_ref[:, cols] = summed * gain_col
        gain_sum = gain_sum + summed * wq_mine[:, cols].astype(jnp.float32)
    go_ref[...] = gathered(3)
    gg_ref[...] = to_row(jnp.sum(gain_sum, axis=1, keepdims=True))
    for copy in pending:
        copy.wait_send()


def stored(gq_ref, go_ref, gg_ref, gq_out, go_out, gg_out, sem):
    copies = []
    for slot, (source, target) in enumerate(
        ((gq_ref, gq_out), (go_ref, go_out), (gg_ref, gg_out))
    ):
        copy = pltpu.make_async_copy(source, target, sem.at[slot])
        copy.start()
        copies.append(copy)
    for copy in copies:
        copy.wait()


def one_kernel(n, replicas, tokens, cotangent, doc_ids, valid_len, w_qkv, w_out, norm_gain):
    rows, width = tokens.shape
    owned, wide = w_qkv.shape
    head = w_out.shape[1]
    chips = n // CORES
    piece = owned // replicas
    vmem = pl.BlockSpec(memory_space=pltpu.VMEM)
    hbm = pl.BlockSpec(memory_space=pltpu.HBM)
    low = jnp.bfloat16
    sem = pltpu.SemaphoreType.DMA
    shapes = (
        jax.ShapeDtypeStruct((owned, wide), jnp.float32),
        jax.ShapeDtypeStruct((owned, head), jnp.float32),
        jax.ShapeDtypeStruct((1, owned), jnp.float32),
    )

    grads = pl.pallas_call(
        functools.partial(fused, n, replicas),
        out_shape=shapes,
        in_specs=[hbm] * 7,
        out_specs=(vmem, vmem, vmem),
        scratch_shapes=[
            pltpu.VMEM((rows, width), low),
            pltpu.VMEM((rows, width), low),
            pltpu.VMEM(doc_ids.shape, jnp.int32),
            pltpu.SMEM(valid_len.shape, jnp.int32),
            pltpu.VMEM((owned,), low),
            pltpu.VMEM((width, wide), low),
            pltpu.VMEM((width, head), low),
            pltpu.VMEM((n, 1, owned), jnp.float32),
            pltpu.VMEM((rows, width), low),
            pltpu.VMEM((chips, rows, owned), low),
            pltpu.VMEM((chips * owned, CORES * rows), low),
            pltpu.VMEM((CORES * rows, head), low),
            pltpu.VMEM((n * rows, owned), low),
            pltpu.VMEM((owned, n * rows), low),
            pltpu.VMEM((3, n * rows, head), low),
            pltpu.VMEM((chips, replicas, piece, head), low),
            pltpu.VMEM((replicas - 1, chips, piece, head), low),
            pltpu.VMEM((chips, piece, head), low),
            pltpu.VMEM((chips - 1, piece, head), low),
            pltpu.VMEM((3, owned, head), low),
            pltpu.VMEM((3, replicas - 1, piece, head), low),
            pltpu.VMEM((4, owned, head), low),
            sem((7,)),
            sem((n + 1, 3)),
            sem((n + 1, 3)),
            sem((n,)),
            sem((n,)),
            sem((n - 1,)),
            sem((n - 1,)),
            sem((chips + 1,)),
            sem((chips + 1,)),
            sem((replicas,)),
            sem((replicas,)),
            sem((chips - 1,)),
            sem((chips - 1,)),
            sem((3, n - 1)),
            sem((3, n - 1)),
            sem((3, replicas)),
            sem((3, replicas)),
            sem((4, replicas)),
            sem((4, replicas)),
        ],
        compiler_params=pltpu.CompilerParams(
            collective_id=0, has_side_effects=True, vmem_limit_bytes=32 * 1024 * 1024
        ),
    )(
        *(
            pltpu.with_memory_space_constraint(array, pltpu.HBM)
            for array in (tokens, cotangent, doc_ids, valid_len, w_qkv, w_out, norm_gain)
        )
    )
    grad_qkv, grad_out, grad_gain = pl.pallas_call(
        stored,
        out_shape=shapes,
        in_specs=[vmem] * 3,
        out_specs=(hbm,) * 3,
        scratch_shapes=[sem((3,))],
        compiler_params=pltpu.CompilerParams(vmem_limit_bytes=4 * 1024 * 1024),
    )(*grads)
    return grad_qkv, grad_out, grad_gain.reshape(owned)


def shards_or_kernel(
    n, replicas, tokens, cotangent, doc_ids, valid_len, w_qkv, w_out, norm_gain
):
    rows, owned, head = tokens.shape[0], w_qkv.shape[0], w_out.shape[1]
    fits = (
        n == 4 * CORES
        and replicas > 1
        and owned % LANES == 0
        and owned % (16 * replicas) == 0
        and rows % LANES == 0
        and rows * n <= 2048
        and head == LANES
        and doc_ids.shape[1] % 8 == 0
    )
    if not fits:
        return shards(tokens, cotangent, doc_ids, valid_len, w_qkv, w_out, norm_gain)
    return one_kernel(
        n, replicas, tokens, cotangent, doc_ids, valid_len, w_qkv, w_out, norm_gain
    )


def solution(mesh):
    in_specs = (
        P(("dp", "rep"), None),
        P(("dp", "rep"), None),
        P(("dp", "rep"), None),
        P(("dp", "rep")),
        P("dp", None),
        P("dp", None),
        P("dp"),
    )
    out_specs = (P("dp", None), P("dp", None), P("dp"))
    body = functools.partial(shards_or_kernel, mesh.shape["dp"], mesh.shape["rep"])
    return jax.shard_map(body, mesh=mesh, in_specs=in_specs, out_specs=out_specs, check_vma=False)
```

```python
import functools
import math

import jax
import jax.numpy as jnp
from jax import lax
from jax.experimental import pallas as pl
from jax.experimental.pallas import tpu as pltpu
from jax.sharding import PartitionSpec as P

NORM_EPS = 1e-06
ROPE_BASE = 1000000.0


def rotate(vector):
    half_size = vector.shape[-1] // 2
    return jnp.concatenate([-vector[..., half_size:], vector[..., :half_size]], axis=-1)


def unrotate(vector):
    half_size = vector.shape[-1] // 2
    return jnp.concatenate([vector[..., half_size:], -vector[..., :half_size]], axis=-1)


def tables(doc_rows, head_size):
    seq_length = doc_rows.shape[1]
    earlier = jnp.sum((doc_rows[:, None, :] < doc_rows[:, :, None]).astype(jnp.int32), axis=2)
    offsets = (jnp.arange(seq_length, dtype=jnp.int32)[None, :] - earlier).astype(jnp.float32)
    frequency = ROPE_BASE ** (-2.0 * jnp.arange(head_size // 2, dtype=jnp.float32) / head_size)
    angles = offsets[:, :, None] * frequency
    angles = jnp.concatenate([angles, angles], axis=2)
    return (jnp.cos(angles), jnp.sin(angles))


def forward_pass(inputs, doc_rows, w_qkv_full, gain_full):
    batches, seq_length, model_width = inputs.shape
    head_size = w_qkv_full.shape[1] // 3
    scale = 1.0 / math.sqrt(head_size)
    wide_in = inputs.astype(jnp.float32)
    inverse_rms = lax.rsqrt(jnp.mean(wide_in * wide_in, axis=2, keepdims=True) + NORM_EPS)
    scaled_in = wide_in * inverse_rms
    normed = (scaled_in * gain_full.astype(jnp.float32)).astype(jnp.bfloat16)
    projected = jnp.dot(
        normed.reshape(-1, model_width), w_qkv_full, preferred_element_type=jnp.float32
    )
    projected = projected.reshape(batches, seq_length, 3 * head_size)
    cosine, sine_part = tables(doc_rows, head_size)
    queries = projected[:, :, :head_size]
    keys_raw = projected[:, :, head_size : 2 * head_size]
    values_raw = projected[:, :, 2 * head_size :]
    query_rot = ((queries * cosine + rotate(queries) * sine_part) * scale).astype(jnp.bfloat16)
    key_rot = (keys_raw * cosine + rotate(keys_raw) * sine_part).astype(jnp.bfloat16)
    values = values_raw.astype(jnp.bfloat16)
    scores = jnp.einsum("msh,mth->mst", query_rot, key_rot, preferred_element_type=jnp.float32)
    order_row = jnp.arange(seq_length, dtype=jnp.int32)[:, None]
    order_col = jnp.arange(seq_length, dtype=jnp.int32)[None, :]
    allowed = (doc_rows[:, :, None] == doc_rows[:, None, :]) & (order_col <= order_row)[None]
    raised = jnp.where(allowed, jnp.exp(scores), 0.0)
    probabilities = raised / jnp.sum(raised, axis=2, keepdims=True)
    probs_low = probabilities.astype(jnp.bfloat16)
    attended = jnp.einsum(
        "mst,mth->msh", probs_low, values, preferred_element_type=jnp.float32
    ).astype(jnp.bfloat16)
    return (
        scaled_in,
        normed,
        query_rot,
        key_rot,
        values,
        probabilities,
        probs_low,
        attended,
        cosine,
        sine_part,
    )


def backward_pass(saved, live_dy, w_qkv_full, w_out_full):
    (
        scaled_in,
        normed,
        query_rot,
        key_rot,
        values,
        probabilities,
        probs_low,
        attended,
        cosine,
        sine_part,
    ) = saved
    batches, seq_length, model_width = live_dy.shape
    head_size = w_out_full.shape[1]
    scale = 1.0 / math.sqrt(head_size)
    d_attended = jnp.dot(
        live_dy.reshape(-1, model_width), w_out_full, preferred_element_type=jnp.float32
    )
    d_attended = d_attended.reshape(batches, seq_length, head_size).astype(jnp.bfloat16)
    d_probs = jnp.einsum("msh,mth->mst", d_attended, values, preferred_element_type=jnp.float32)
    d_values = jnp.einsum("mst,msh->mth", probs_low, d_attended, preferred_element_type=jnp.float32)
    d_scores = (
        probabilities * (d_probs - jnp.sum(probabilities * d_probs, axis=2, keepdims=True))
    ).astype(jnp.bfloat16)
    d_query = (
        jnp.einsum("mst,mth->msh", d_scores, key_rot, preferred_element_type=jnp.float32) * scale
    )
    d_key = jnp.einsum("mst,msh->mth", d_scores, query_rot, preferred_element_type=jnp.float32)
    d_query = d_query * cosine + unrotate(d_query * sine_part)
    d_key = d_key * cosine + unrotate(d_key * sine_part)
    d_qkv = jnp.concatenate([d_query, d_key, d_values], axis=2).astype(jnp.bfloat16)
    d_normed = lax.dot_general(
        d_qkv.reshape(-1, 3 * head_size),
        w_qkv_full,
        (((1,), (1,)), ((), ())),
        preferred_element_type=jnp.float32,
    )
    gain_term = jnp.sum(d_normed * scaled_in.reshape(-1, model_width), axis=0)
    return (d_qkv, gain_term)


def shards(tokens, cotangent, doc_ids, valid_len, w_qkv, w_out, norm_gain):
    batches, seq_length = doc_ids.shape
    model_width = tokens.shape[1]
    inputs = tokens.reshape(batches, seq_length, model_width)
    live_rows = jnp.arange(seq_length, dtype=jnp.int32)[None, :] < valid_len[:, None]
    live_dy = jnp.where(
        live_rows[:, :, None],
        cotangent.reshape(batches, seq_length, model_width),
        jnp.zeros((), jnp.bfloat16),
    )
    full_set = (
        lax.all_gather(w_qkv, "dp", axis=0, tiled=True),
        lax.all_gather(w_out, "dp", axis=0, tiled=True),
        lax.all_gather(norm_gain, "dp", axis=0, tiled=True),
    )
    saved = forward_pass(inputs, doc_ids, full_set[0], full_set[2])
    qkv_all, gain_total = backward_pass(saved, live_dy, full_set[0], full_set[1])
    normed_all = saved[1]
    attended_all = saved[7]
    head_size = w_out.shape[1]
    normed_flat = normed_all.reshape(-1, model_width)
    qkv_flat = qkv_all.reshape(-1, 3 * head_size)
    attended_flat = attended_all.reshape(-1, head_size)
    grad_qkv = lax.dot_general(
        normed_flat, qkv_flat, (((0,), (0,)), ((), ())), preferred_element_type=jnp.float32
    )
    grad_out = lax.dot_general(
        live_dy.reshape(-1, model_width),
        attended_flat,
        (((0,), (0,)), ((), ())),
        preferred_element_type=jnp.float32,
    )
    shares = (
        lax.psum_scatter(grad_qkv, "dp", scatter_dimension=0, tiled=True),
        lax.psum_scatter(grad_out, "dp", scatter_dimension=0, tiled=True),
    )
    shares = lax.psum((shares[0], shares[1]), "rep")
    gain_whole = lax.psum(gain_total, ("dp", "rep"))
    owned_rows = w_qkv.shape[0]
    gain_start = lax.axis_index("dp") * owned_rows
    gain_owned = lax.dynamic_slice_in_dim(gain_whole, gain_start, owned_rows, 0)
    replicas = lax.axis_size("rep")
    return (shares[0] / replicas, shares[1] / replicas, gain_owned / replicas)


MESH = pl.DeviceIdType.MESH
LANES = 128
CORES = 2


def mm(left, right, dims):
    return lax.dot_general(left, right, (dims, ((), ())), preferred_element_type=jnp.float32)


def eye(size):
    return lax.broadcasted_iota(jnp.int32, (size, size), 0) == lax.broadcasted_iota(
        jnp.int32, (size, size), 1
    )


def to_column(row):
    return jnp.sum(jnp.where(eye(row.shape[1]), row, 0.0), axis=1, keepdims=True)


def to_row(column):
    return jnp.sum(jnp.where(eye(column.shape[0]), column, 0.0), axis=0, keepdims=True)


def fused(
    n,
    replicas,
    x_hbm,
    dy_hbm,
    doc_hbm,
    valid_hbm,
    wq_hbm,
    wo_hbm,
    gain_hbm,
    gq_ref,
    go_ref,
    gg_ref,
    x_v,
    dy_v,
    doc_v,
    valid_s,
    gain_v,
    wq_all,
    wo_all,
    gain_all,
    normed,
    dy_sib,
    dy_turned,
    att,
    x_all,
    x_turned,
    y_all,
    p_send,
    p_recv,
    q_send,
    q_recv,
    z_send,
    z_recv,
    z_all,
    z_sums,
    o_all,
    in_sem,
    sent_sem,
    one_sem,
    w_sem,
    y_sem,
    r_sem,
    g_sem,
):
    me = lax.axis_index("dp")
    rep = lax.axis_index("rep")
    chip, core = me // CORES, lax.rem(me, CORES)
    sibling = chip * CORES + (1 - core)
    rows, width = x_v.shape
    owned = wq_hbm.shape[0]
    head = wo_hbm.shape[1]
    chips = n // CORES
    samples, seq = doc_v.shape
    piece = owned // replicas
    half_owned = owned // 2
    scale = 1.0 / math.sqrt(head)

    def block(index, size):
        return pl.ds(pl.multiple_of(index * size, LANES), size)

    loads = []
    for slot, (source, target) in enumerate(
        (
            (wq_hbm, wq_all.at[block(me, owned)]),
            (wo_hbm, wo_all.at[block(me, owned)]),
            (gain_hbm, gain_v),
            (x_hbm, x_v),
            (dy_hbm, dy_v),
            (doc_hbm, doc_v),
            (valid_hbm, valid_s),
        )
    ):
        load = pltpu.make_async_copy(source, target, in_sem.at[slot])
        load.start()
        loads.append(load)

    barrier = pltpu.get_barrier_semaphore()
    for off in range(1, n):
        pl.semaphore_signal(
            barrier, inc=1, device_id={"dp": lax.rem(me + off, n)}, device_id_type=MESH
        )
    for off in range(1, replicas):
        pl.semaphore_signal(
            barrier,
            inc=1,
            device_id={"rep": lax.rem(rep + off, replicas)},
            device_id_type=MESH,
        )

    GAIN, X, DY, ATT, PARTS, PIECES, OUT, WQ, WO, Y, SUMS, DONE = range(12)

    def remote(src, dst, group, recv_sem, where):
        return pltpu.make_async_remote_copy(
            src_ref=src,
            dst_ref=dst,
            send_sem=sent_sem.at[group],
            recv_sem=recv_sem,
            device_id=where,
            device_id_type=MESH,
        )

    def send(src, dst, group, recv_sem, where):
        remote(src, dst, group, recv_sem, where).start()

    def landed(ref, recv_sem):
        remote(ref, ref, 0, recv_sem, {"dp": sibling}).wait_recv()

    def left(ref, group):
        remote(ref, ref, group, one_sem.at[0], {"dp": sibling}).wait_send()

    along, across = lax.rem(chip, 2), chip // 2
    by_x = across * 2 + 1 - along
    by_y = (1 - across) * 2 + along
    first = by_x + core * (by_y - by_x)
    second = by_y + core * (by_x - by_y)
    far = 3 - chip
    owners = (
        first * CORES + core,
        second * CORES + core,
        far * CORES + core,
        sibling,
        second * CORES + 1 - core,
        first * CORES + 1 - core,
        far * CORES + 1 - core,
    )

    def w_part(owner, part):
        if part == 2:
            return wo_all.at[block(owner, owned)]
        start = pl.multiple_of(owner * owned + part * half_owned, LANES)
        return wq_all.at[pl.ds(start, half_owned)]

    arrivals = {
        (0, 0): 0,
        (0, 1): 1,
        (0, 2): 2,
        (1, 0): 3,
        (1, 2): 4,
        (2, 0): 5,
        (2, 1): 6,
        (2, 2): 7,
        (3, 0): 8,
        (3, 1): 8,
        (4, 0): 9,
        (4, 1): 9,
        (5, 0): 10,
        (8, 0): 10,
        (6, 0): 11,
        (6, 1): 11,
        (7, 0): 12,
        (7, 2): 13,
        (3, 2): 14,
        (4, 2): 14,
        (5, 2): 14,
        (8, 2): 14,
        (6, 2): 14,
    }

    def w_send(source, slot, part, where):
        group = WO if part == 2 else WQ
        send(source, source, group, w_sem.at[arrivals[slot, part]], where)

    def w_copy(owner, part, slot, device):
        w_send(w_part(owner, part), slot, part, {"dp": device})

    def w_landed(slot, part, size):
        landed((wo_all if part == 2 else wq_all).at[:size], w_sem.at[arrivals[slot, part]])

    side = lax.rem(rep, 2)
    partner = rep + 1 - 2 * side

    def w_half(owner, part, which):
        start = pl.multiple_of(owner * owned + which * half_owned, LANES)
        return (wo_all if part == 2 else wq_all).at[pl.ds(start, half_owned)]

    def half_copy(owner, part, which, slot, where):
        w_send(w_half(owner, part, which), slot, part, where)

    loads[2].wait()
    gain_row = gain_v[...].reshape(1, owned).astype(jnp.float32)
    gain_all[me] = gain_row
    loads[0].wait()
    loads[1].wait()
    pl.semaphore_wait(barrier, n - 1 + replicas - 1)

    for off in range(1, n):
        send(
            gain_all.at[me],
            gain_all.at[me],
            GAIN,
            one_sem.at[GAIN],
            {"dp": lax.rem(me + off, n)},
        )
    for part in range(2):
        w_copy(me, part, 0, owners[0])
    for part in range(2):
        w_copy(me, part, 3, sibling)
    w_copy(me, 2, 3, sibling)

    loads[4].wait()
    for place in range(chips):
        send(
            dy_v.at[:, block(place * CORES + 1 - core, owned)],
            dy_sib.at[place],
            DY,
            one_sem.at[DY],
            {"dp": sibling},
        )

    loads[3].wait()
    loads[5].wait()
    loads[6].wait()
    gain_col = to_column(gain_row)
    wide_in = x_v[...].astype(jnp.float32)
    inverse = lax.rsqrt(
        jnp.sum(wide_in * wide_in, axis=1, keepdims=True) * (1.0 / width) + NORM_EPS
    )
    keys, live = [], []
    for m in range(samples):
        doc_row = doc_v[m : m + 1, :].astype(jnp.float32)
        keys.append(to_column(doc_row) + float(m * seq))
        place = lax.broadcasted_iota(jnp.int32, (seq, 1), 0)
        live.append(jnp.where(place < valid_s[m], 1.0, 0.0))
    key_col = jnp.concatenate(keys, axis=0)
    live_col = jnp.concatenate(live, axis=0)
    key_row = to_row(key_col)
    earlier = jnp.sum(jnp.where(key_row < key_col, 1.0, 0.0), axis=1, keepdims=True)
    order_row = lax.broadcasted_iota(jnp.int32, (rows, rows), 0)
    order_col = lax.broadcasted_iota(jnp.int32, (rows, rows), 1)
    allowed = (key_row == key_col) & (order_col <= order_row)
    offsets = lax.broadcasted_iota(jnp.int32, (rows, 1), 0).astype(jnp.float32) - earlier
    lane = lax.broadcasted_iota(jnp.int32, (1, head), 1)
    half = lax.rem(lane, head // 2).astype(jnp.float32)
    frequency = jnp.exp(half * (-2.0 / head * math.log(ROPE_BASE)))
    angles = offsets * frequency
    cosine = jnp.cos(angles)
    signed = jnp.sin(angles) * jnp.where(lane < head // 2, -1.0, 1.0)

    for part in (0, 2):
        half_copy(me, part, side, 1, {"dp": owners[1]})
    w_copy(me, 2, 0, owners[0])
    mine = block(me, rows)

    def x_copy(slot):
        send(
            x_v.at[:, block(owners[slot], owned)],
            x_all.at[mine],
            X,
            one_sem.at[X],
            {"dp": owners[slot]},
        )

    for slot in (3, 0, 5, 1):
        x_copy(slot)
    landed(gain_all.at[: n - 1], one_sem.at[GAIN])
    for place in range(n):
        cols = pl.ds(place * owned, owned)
        scaled = x_v[:, cols].astype(jnp.float32) * inverse
        normed[:, cols] = (scaled * gain_all[place]).astype(jnp.bfloat16)

    def times(source, total):
        product = mm(normed[:, block(source, owned)], wq_all[block(source, owned), :], ((1,), (0,)))
        return product if total is None else total + product

    total = times(me, None)
    w_landed(3, 0, owned)
    total = times(sibling, total)

    for part in range(2):
        w_landed(0, part, half_owned)
        w_copy(owners[0], part, 2, owners[1])
        w_copy(owners[0], part, 4, sibling)
    for part in (0, 2):
        w_landed(1, part, half_owned)
        half_copy(owners[1], part, side, 7, {"rep": partner})
        half_copy(owners[1], part, side, 5, {"dp": sibling})

    landed(dy_sib, one_sem.at[DY])
    for place in range(chips):
        turned = pl.ds(place * owned, owned)
        dy_turned[turned, :rows] = dy_v[:, block(place * CORES + core, owned)].T
        dy_turned[turned, rows:] = dy_sib[place].T

    total = times(owners[0], total)

    w_landed(0, 2, owned)
    w_copy(owners[0], 2, 2, owners[1])
    w_copy(owners[0], 2, 4, sibling)
    for slot in (2, 6, 4):
        x_copy(slot)

    w_landed(4, 0, owned)
    total = times(owners[4], total)
    for part in range(2):
        w_landed(2, part, half_owned)
        w_copy(owners[2], part, 6, sibling)
    for part in (0, 2):
        w_landed(7, part, half_owned)
        half_copy(owners[1], part, 1 - side, 8, {"dp": sibling})

    total = times(owners[1], total)
    total = times(owners[2], total)
    w_landed(2, 2, owned)
    w_copy(owners[2], 2, 6, sibling)
    w_landed(5, 0, owned)
    total = times(owners[5], total)
    w_landed(6, 0, owned)
    projected = times(owners[6], total)

    def turn(vector, sine_part):
        return vector * cosine + pltpu.roll(vector, head // 2, 1) * sine_part

    query = (turn(projected[:, :head], signed) * scale).astype(jnp.bfloat16)
    key = turn(projected[:, head : 2 * head], signed).astype(jnp.bfloat16)
    values = projected[:, 2 * head :].astype(jnp.bfloat16)
    scores = mm(query, key, ((1,), (1,)))
    raised = jnp.where(allowed, jnp.exp(scores), 0.0)
    probs = raised / jnp.sum(raised, axis=1, keepdims=True)
    probs_low = probs.astype(jnp.bfloat16)
    attended = mm(probs_low, values, ((1,), (0,)))
    att[:rows] = (attended * live_col).astype(jnp.bfloat16)
    send(att.at[:rows], att.at[rows:], ATT, one_sem.at[ATT], {"dp": sibling})
    w_landed(3, 2, chips * owned)
    d_att = (mm(dy_v[...], wo_all[...], ((1,), (0,))) * live_col).astype(jnp.bfloat16)
    landed(att.at[rows:], one_sem.at[ATT])

    by_chip = mm(dy_turned[...], att[...], ((1,), (0,)))
    p_send[...] = by_chip.reshape(chips, replicas, piece, head).astype(jnp.bfloat16)
    for off in range(1, replicas):
        peer = lax.rem(rep + off, replicas)
        send(p_send.at[:, peer], p_recv.at[off - 1], PARTS, one_sem.at[PARTS], {"rep": peer})

    def y_copy(chunk, owner, slot, device):
        source = y_all.at[chunk].at[block(owner, rows)]
        send(source, source, Y, y_sem.at[chunk, min(slot, 3)], {"dp": device})

    def y_start(chunk, value):
        y_all[chunk, mine] = (value * inverse).astype(jnp.bfloat16)
        for slot in (2, 0, 1, 3):
            y_copy(chunk, me, slot, owners[slot])

    y_start(0, mm(probs_low, d_att, ((0,), (0,))))
    d_probs = mm(d_att, values, ((1,), (1,)))
    d_scores = (
        probs * (d_probs - jnp.sum(probs * d_probs, axis=1, keepdims=True))
    ).astype(jnp.bfloat16)
    y_start(1, turn(mm(d_scores, key, ((1,), (0,))) * scale, -signed))
    y_start(2, turn(mm(d_scores, query, ((0,), (0,))), -signed))

    x_turned[:, mine] = x_v[:, block(me, owned)].T
    landed(x_all.at[: (n - 1) * rows], one_sem.at[X])
    for owner in owners:
        part = block(owner, rows)
        x_turned[:, part] = x_all[part].T

    my_piece = pl.ds(pl.multiple_of(rep * piece, 16), piece)

    def y_pass(chunk):
        for slot, onward in ((2, 6), (0, 4), (1, 5)):
            landed(y_all.at[chunk].at[:rows], y_sem.at[chunk, slot])
            y_copy(chunk, owners[slot], onward, sibling)

    lead = replicas // 2 - 1
    near = rep // (replicas // 2)
    central = (rep == lead) | (rep == lead + 1)
    summing = central & (core == 1)
    head_core = chip * CORES + 1

    def half_rows(which):
        return pl.ds(pl.multiple_of(which * half_owned, LANES), half_owned)

    def to_center(chunk, which):
        send(
            z_send.at[chunk].at[half_rows(which)],
            z_recv.at[chunk, core, rep],
            SUMS,
            r_sem.at[chunk, core],
            {"dp": head_core, "rep": lead + which},
        )

    def y_finish(chunk):
        landed(y_all.at[chunk].at[: chips * rows], y_sem.at[chunk, 3])
        total = mm(x_turned[...], y_all[chunk], ((1,), (0,)))
        z_send[chunk] = total.astype(jnp.bfloat16)
        to_center(chunk, 1 - near)

        @pl.when(jnp.logical_not(summing))
        def _():
            to_center(chunk, near)

    def z_gather(whole):
        o_all[my_piece] = (whole * (1.0 / replicas)).astype(jnp.bfloat16)
        for off in range(1, replicas):
            send(
                o_all.at[my_piece],
                o_all.at[my_piece],
                OUT,
                one_sem.at[OUT],
                {"rep": lax.rem(rep + off, replicas)},
            )

    def from_center(chunk, place, off):
        rows_here = z_all.at[chunk].at[half_rows(near)]
        send(
            rows_here if place == 1 else z_sums.at[chunk],
            rows_here,
            DONE,
            g_sem.at[chunk, near],
            {"dp": chip * CORES + place, "rep": lax.rem(rep + off, replicas)},
        )

    def z_sum(chunk):
        @pl.when(summing)
        def _():
            for place in range(CORES):
                if place == 1:
                    landed(z_recv.at[chunk, 1].at[: replicas - 1], r_sem.at[chunk, 1])
                    whole = z_send[chunk, half_rows(near)].astype(jnp.float32)
                else:
                    landed(z_recv.at[chunk, 0], r_sem.at[chunk, 0])
                    whole = z_recv[chunk, 0, rep].astype(jnp.float32)
                for off in range(1, replicas):
                    source = lax.rem(rep + off, replicas)
                    whole = whole + z_recv[chunk, place, source].astype(jnp.float32)
                low = (whole * (1.0 / replicas)).astype(jnp.bfloat16)
                if place == 1:
                    z_all[chunk, half_rows(near)] = low
                else:
                    z_sums[chunk] = low
                for off in (2, 3, 1) if place == 1 else (2, 3, 1, 0):
                    from_center(chunk, place, off)

    def z_arrived(chunk, which):
        landed(z_all.at[chunk].at[:half_owned], g_sem.at[chunk, which])

    def z_done(chunk):
        @pl.when(jnp.logical_not(summing))
        def _():
            z_arrived(chunk, near)

        z_arrived(chunk, 1 - near)
        return z_all[chunk].astype(jnp.float32)

    y_pass(0)
    y_pass(1)
    y_finish(0)
    y_pass(2)
    y_finish(1)
    y_finish(2)
    q_whole = p_send[:, rep].astype(jnp.float32)
    landed(p_recv, one_sem.at[PARTS])
    for off in range(1, replicas):
        q_whole = q_whole + p_recv[off - 1].astype(jnp.float32)
    q_send[...] = q_whole.astype(jnp.bfloat16)
    for slot in range(chips - 1):
        send(
            q_send.at[owners[slot] // CORES],
            q_recv.at[slot],
            PIECES,
            one_sem.at[PIECES],
            {"dp": owners[slot]},
        )
    z_sum(0)
    z_sum(1)
    whole = q_send[chip].astype(jnp.float32)
    landed(q_recv, one_sem.at[PIECES])
    for slot in range(chips - 1):
        whole = whole + q_recv[slot].astype(jnp.float32)
    z_gather(whole)
    z_sum(2)
    others = (n - 1) * owned
    left(gain_all.at[: n - 1], GAIN)
    left(x_all.at[: (n - 1) * rows], X)
    left(dy_sib, DY)
    left(att.at[rows:], ATT)
    left(p_recv, PARTS)
    left(q_recv, PIECES)
    left(wq_all.at[:others], WQ)
    left(wo_all.at[:others], WO)
    left(y_all.at[:, : (n - 1) * rows], Y)

    wq_mine = wq_all.at[block(me, owned)]
    gain_sum = None
    for chunk, place in ((0, 2), (1, 0), (2, 1)):
        if chunk == 2:
            landed(o_all.at[: (replicas - 1) * piece], one_sem.at[OUT])
            go_ref[...] = o_all[...].astype(jnp.float32)
        cols = pl.ds(place * head, head)
        summed = z_done(chunk)
        gq_ref[:, cols] = summed * gain_col
        term = summed * wq_mine[:, cols].astype(jnp.float32)
        gain_sum = term if gain_sum is None else gain_sum + term
    gg_ref[...] = to_row(jnp.sum(gain_sum, axis=1, keepdims=True))
    left(o_all.at[: (replicas - 1) * piece], OUT)

    @pl.when(jnp.logical_not(summing))
    def _():
        left(z_send, SUMS)

    @pl.when(summing)
    def _():
        left(z_send.at[:, :half_owned], SUMS)
        left(y_all.at[:, : (2 * replicas - 1) * half_owned], DONE)


def stored(gq_ref, go_ref, gg_ref, gq_out, go_out, gg_out, sem):
    copies = []
    for slot, (source, target) in enumerate(
        ((gq_ref, gq_out), (go_ref, go_out), (gg_ref, gg_out))
    ):
        copy = pltpu.make_async_copy(source, target, sem.at[slot])
        copy.start()
        copies.append(copy)
    for copy in copies:
        copy.wait()


def one_kernel(n, replicas, tokens, cotangent, doc_ids, valid_len, w_qkv, w_out, norm_gain):
    rows, width = tokens.shape
    owned, wide = w_qkv.shape
    head = w_out.shape[1]
    chips = n // CORES
    piece = owned // replicas
    vmem = pl.BlockSpec(memory_space=pltpu.VMEM)
    hbm = pl.BlockSpec(memory_space=pltpu.HBM)
    low = jnp.bfloat16
    sem = pltpu.SemaphoreType.DMA
    shapes = (
        jax.ShapeDtypeStruct((owned, wide), jnp.float32),
        jax.ShapeDtypeStruct((owned, head), jnp.float32),
        jax.ShapeDtypeStruct((1, owned), jnp.float32),
    )

    grads = pl.pallas_call(
        functools.partial(fused, n, replicas),
        out_shape=shapes,
        in_specs=[hbm] * 7,
        out_specs=(vmem, vmem, vmem),
        scratch_shapes=[
            pltpu.VMEM((rows, width), low),
            pltpu.VMEM((rows, width), low),
            pltpu.VMEM(doc_ids.shape, jnp.int32),
            pltpu.SMEM(valid_len.shape, jnp.int32),
            pltpu.VMEM((owned,), low),
            pltpu.VMEM((width, wide), low),
            pltpu.VMEM((width, head), low),
            pltpu.VMEM((n, 1, owned), jnp.float32),
            pltpu.VMEM((rows, width), low),
            pltpu.VMEM((chips, rows, owned), low),
            pltpu.VMEM((chips * owned, CORES * rows), low),
            pltpu.VMEM((CORES * rows, head), low),
            pltpu.VMEM((n * rows, owned), low),
            pltpu.VMEM((owned, n * rows), low),
            pltpu.VMEM((3, n * rows, head), low),
            pltpu.VMEM((chips, replicas, piece, head), low),
            pltpu.VMEM((replicas - 1, chips, piece, head), low),
            pltpu.VMEM((chips, piece, head), low),
            pltpu.VMEM((chips - 1, piece, head), low),
            pltpu.VMEM((3, owned, head), low),
            pltpu.VMEM((3, CORES, replicas, owned // 2, head), low),
            pltpu.VMEM((3, owned, head), low),
            pltpu.VMEM((3, owned // 2, head), low),
            pltpu.VMEM((owned, head), low),
            sem((7,)),
            sem((12,)),
            sem((7,)),
            sem((15,)),
            sem((3, 4)),
            sem((3, CORES)),
            sem((3, 2)),
        ],
        compiler_params=pltpu.CompilerParams(
            collective_id=0, has_side_effects=True, vmem_limit_bytes=32 * 1024 * 1024
        ),
    )(
        *(
            pltpu.with_memory_space_constraint(array, pltpu.HBM)
            for array in (tokens, cotangent, doc_ids, valid_len, w_qkv, w_out, norm_gain)
        )
    )
    grad_qkv, grad_out, grad_gain = pl.pallas_call(
        stored,
        out_shape=shapes,
        in_specs=[vmem] * 3,
        out_specs=(hbm,) * 3,
        scratch_shapes=[sem((3,))],
        compiler_params=pltpu.CompilerParams(vmem_limit_bytes=4 * 1024 * 1024),
    )(*grads)
    return grad_qkv, grad_out, grad_gain.reshape(owned)


def shards_or_kernel(
    n, replicas, tokens, cotangent, doc_ids, valid_len, w_qkv, w_out, norm_gain
):
    rows, owned, head = tokens.shape[0], w_qkv.shape[0], w_out.shape[1]
    fits = (
        n == 4 * CORES
        and replicas == 4
        and owned % LANES == 0
        and owned % (2 * LANES) == 0
        and rows % LANES == 0
        and rows * n <= 2048
        and head == LANES
        and doc_ids.shape[1] % 8 == 0
    )
    if not fits:
        return shards(tokens, cotangent, doc_ids, valid_len, w_qkv, w_out, norm_gain)
    return one_kernel(
        n, replicas, tokens, cotangent, doc_ids, valid_len, w_qkv, w_out, norm_gain
    )


def solution(mesh):
    in_specs = (
        P(("dp", "rep"), None),
        P(("dp", "rep"), None),
        P(("dp", "rep"), None),
        P(("dp", "rep")),
        P("dp", None),
        P("dp", None),
        P("dp"),
    )
    out_specs = (P("dp", None), P("dp", None), P("dp"))
    body = functools.partial(shards_or_kernel, mesh.shape["dp"], mesh.shape["rep"])
    return jax.shard_map(body, mesh=mesh, in_specs=in_specs, out_specs=out_specs, check_vma=False)
```
